16 devices in a mesh: dp: 2 (over y, z), sp: 8 (over x, core).
Axes of the slice: x: 4, y: 2, z: 1, core: 2. Of those that a mesh axis runs over, the one named last changes fastest.
The devices are a block of a 4x4x8 slice.
Arguments:
- hidden: bfloat16 [12288, 2048], P(('dp', 'sp')), parts along dimension 0
- positions: int32 [12288], P(('dp', 'sp')), parts along dimension 0
- d_attn: bfloat16 [12288, 2048], P(('dp', 'sp')), parts along dimension 0
- ln_weight: bfloat16 [2048], replicated
- w_q: bfloat16 [2048, 2048], replicated
- w_k: bfloat16 [2048, 2048], replicated
- w_v: bfloat16 [2048, 2048], replicated
- w_o: bfloat16 [2048, 2048], replicated
Outputs:
- output 1: bfloat16 [12288, 2048], P(('dp', 'sp')), parts along dimension 0
- output 2: bfloat16 [12288, 2048], P(('dp', 'sp')), parts along dimension 0
- output 3: bfloat16 [4096], P('dp'), parts along dimension 0
- output 4: bfloat16 [4096, 2048], P('dp'), parts along dimension 0
- output 5: bfloat16 [4096, 2048], P('dp'), parts along dimension 0
- output 6: bfloat16 [4096, 2048], P('dp'), parts along dimension 0
- output 7: bfloat16 [4096, 2048], P('dp'), parts along dimension 0
There are 2 independent parts. The reference program is written for one: setup_inputs(seed, part) draws one part's arguments, and reference() takes and returns one part's arrays. A program takes and returns all parts, laid end to end along the dimension named above; an argument that names none is the same for every part.
All inputs are finite; a program needn't handle non-finite values.
Results may differ from the reference program's by a relative error of at most 0.0122721.
Values are sent between devices in bfloat16 or wider.
A program may use at most 768 MiB of HBM per device.

```python
import math
import jax
import jax.numpy as jnp
from jax import lax

MODEL_DIM = 2048
NUM_HEADS = 16
NUM_KV_HEADS = 16
HEAD_DIM = 128
SEQ_LEN = 6144
LN_EPS = 1e-5
ROPE_BASE = 10000.0
GROUP_SIZE = NUM_HEADS // NUM_KV_HEADS
ROW_BLOCK = math.gcd(SEQ_LEN, 64)
NUM_BLOCKS = SEQ_LEN // ROW_BLOCK
SCORE_SCALE = HEAD_DIM ** -0.5


def setup_inputs(seed: int = 0, part: int = 0) -> dict:
    base_key = jax.random.key(seed)
    part_keys = jax.random.split(jax.random.fold_in(base_key, part), 3)
    weight_keys = jax.random.split(base_key, 5)
    hidden = jax.random.normal(part_keys[0], (SEQ_LEN, MODEL_DIM), jnp.float32).astype(jnp.bfloat16)
    pos_steps = jax.random.randint(part_keys[1], (SEQ_LEN,), 1, 4, dtype=jnp.int32)
    positions = (jnp.cumsum(pos_steps) - pos_steps[0]).astype(jnp.int32)
    d_attn = jax.random.normal(part_keys[2], (SEQ_LEN, MODEL_DIM), jnp.float32).astype(jnp.bfloat16)
    ln_weight = (1.0 + 0.25 * jax.random.normal(weight_keys[0], (MODEL_DIM,), jnp.float32)).astype(jnp.bfloat16)
    q_scale = math.sqrt(math.log(SEQ_LEN) / MODEL_DIM)
    kv_scale = MODEL_DIM ** -0.5
    o_scale = (NUM_HEADS * HEAD_DIM) ** -0.5
    w_q = (jax.random.normal(weight_keys[1], (MODEL_DIM, NUM_HEADS * HEAD_DIM), jnp.float32) * q_scale).astype(jnp.bfloat16)
    w_k = (jax.random.normal(weight_keys[2], (MODEL_DIM, NUM_KV_HEADS * HEAD_DIM), jnp.float32) * kv_scale).astype(jnp.bfloat16)
    w_v = (jax.random.normal(weight_keys[3], (MODEL_DIM, NUM_KV_HEADS * HEAD_DIM), jnp.float32) * kv_scale).astype(jnp.bfloat16)
    w_o = (jax.random.normal(weight_keys[4], (NUM_HEADS * HEAD_DIM, MODEL_DIM), jnp.float32) * o_scale).astype(jnp.bfloat16)
    return {'hidden': hidden, 'positions': positions, 'd_attn': d_attn, 'ln_weight': ln_weight,
            'w_q': w_q, 'w_k': w_k, 'w_v': w_v, 'w_o': w_o}


def norm_f32(hid_f32, weight_f32):
    mean_val = jnp.mean(hid_f32, axis=-1, keepdims=True)
    centered = hid_f32 - mean_val
    var_val = jnp.mean(centered * centered, axis=-1, keepdims=True)
    return centered * lax.rsqrt(var_val + LN_EPS) * weight_f32


def rope_tables(positions):
    inv_freq = ROPE_BASE ** (-jnp.arange(0, HEAD_DIM, 2, dtype=jnp.float32) / HEAD_DIM)
    angles = positions.astype(jnp.float32)[:, None] * inv_freq[None, :]
    return jnp.cos(angles)[:, None, :], jnp.sin(angles)[:, None, :]


def apply_rope(values, cos_t, sin_t):
    rot_pairs = values.reshape(values.shape[:-1] + (HEAD_DIM // 2, 2))
    even_part = rot_pairs[..., 0]
    odd_part = rot_pairs[..., 1]
    new_even = even_part * cos_t - odd_part * sin_t
    new_odd = odd_part * cos_t + even_part * sin_t
    return jnp.stack([new_even, new_odd], axis=-1).reshape(values.shape)


def block_probs(q_f32, row_start, k_f32):
    scores = jnp.einsum('qgrd,kgd->grqk', q_f32, k_f32) * SCORE_SCALE
    row_ids = row_start + jnp.arange(ROW_BLOCK)
    col_ids = jnp.arange(SEQ_LEN)
    scores = jnp.where(row_ids[:, None] >= col_ids[None, :], scores, -jnp.inf)
    return jax.nn.softmax(scores, axis=-1)


def reference(hidden, positions, d_attn, ln_weight, w_q, w_k, w_v, w_o):
    normed32, norm_vjp = jax.vjp(norm_f32, hidden.astype(jnp.float32), ln_weight.astype(jnp.float32))
    normed = normed32.astype(jnp.bfloat16)
    cos_t, sin_t = rope_tables(positions)
    q_rot = apply_rope(jnp.dot(normed, w_q, preferred_element_type=jnp.float32).reshape(SEQ_LEN, NUM_HEADS, HEAD_DIM), cos_t, sin_t).astype(jnp.bfloat16)
    k_rot = apply_rope(jnp.dot(normed, w_k, preferred_element_type=jnp.float32).reshape(SEQ_LEN, NUM_KV_HEADS, HEAD_DIM), cos_t, sin_t).astype(jnp.bfloat16)
    v_all = jnp.dot(normed, w_v, preferred_element_type=jnp.float32).astype(jnp.bfloat16).reshape(SEQ_LEN, NUM_KV_HEADS, HEAD_DIM)
    q_grp = q_rot.reshape(NUM_BLOCKS, ROW_BLOCK, NUM_KV_HEADS, GROUP_SIZE, HEAD_DIM)
    k_f32 = k_rot.astype(jnp.float32)
    v_f32 = v_all.astype(jnp.float32)
    block_ids = jnp.arange(NUM_BLOCKS)

    def fwd_block(block_in):
        q_block, block_idx = block_in
        attn_prob = block_probs(q_block.astype(jnp.float32), block_idx * ROW_BLOCK, k_f32)
        prob_bf = attn_prob.astype(jnp.bfloat16).astype(jnp.float32)
        return jnp.einsum('grqk,kgd->qgrd', prob_bf, v_f32).astype(jnp.bfloat16)

    o_grp = lax.map(fwd_block, (q_grp, block_ids))
    o_tok = o_grp.reshape(SEQ_LEN, NUM_HEADS * HEAD_DIM)
    attn_out = jnp.dot(o_tok, w_o, preferred_element_type=jnp.float32).astype(jnp.bfloat16)
    d_o = jnp.dot(d_attn, w_o.T, preferred_element_type=jnp.float32).astype(jnp.bfloat16)
    dw_o = jnp.dot(o_tok.T, d_attn, preferred_element_type=jnp.float32)
    do_grp = d_o.reshape(NUM_BLOCKS, ROW_BLOCK, NUM_KV_HEADS, GROUP_SIZE, HEAD_DIM)

    def bwd_block(carry, block_in):
        dk_acc, dv_acc = carry
        q_block, do_block, block_idx = block_in
        q_f32 = q_block.astype(jnp.float32)
        do_f32 = do_block.astype(jnp.float32)
        attn_prob = block_probs(q_f32, block_idx * ROW_BLOCK, k_f32)
        prob_bf = attn_prob.astype(jnp.bfloat16).astype(jnp.float32)
        d_prob = jnp.einsum('qgrd,kgd->grqk', do_f32, v_f32)
        row_dot = jnp.sum(attn_prob * d_prob, axis=-1, keepdims=True)
        d_score = (attn_prob * (d_prob - row_dot) * SCORE_SCALE).astype(jnp.bfloat16).astype(jnp.float32)
        dq_block = jnp.einsum('grqk,kgd->qgrd', d_score, k_f32).astype(jnp.bfloat16)
        dk_acc = dk_acc + jnp.einsum('grqk,qgrd->kgd', d_score, q_f32)
        dv_acc = dv_acc + jnp.einsum('grqk,qgrd->kgd', prob_bf, do_f32)
        return (dk_acc, dv_acc), dq_block

    zero_acc = jnp.zeros((SEQ_LEN, NUM_KV_HEADS, HEAD_DIM), jnp.float32)
    kv_sums, dq_grp = lax.scan(bwd_block, (zero_acc, zero_acc), (q_grp, do_grp, block_ids))
    dk_bf = kv_sums[0].astype(jnp.bfloat16)
    dv_bf = kv_sums[1].astype(jnp.bfloat16)
    g_q = apply_rope(dq_grp.reshape(SEQ_LEN, NUM_HEADS, HEAD_DIM).astype(jnp.float32), cos_t, -sin_t).astype(jnp.bfloat16).reshape(SEQ_LEN, NUM_HEADS * HEAD_DIM)
    g_k = apply_rope(dk_bf.astype(jnp.float32), cos_t, -sin_t).astype(jnp.bfloat16).reshape(SEQ_LEN, NUM_KV_HEADS * HEAD_DIM)
    g_v = dv_bf.reshape(SEQ_LEN, NUM_KV_HEADS * HEAD_DIM)
    d_normed = (jnp.dot(g_q, w_q.T, preferred_element_type=jnp.float32)
                + jnp.dot(g_k, w_k.T, preferred_element_type=jnp.float32)
                + jnp.dot(g_v, w_v.T, preferred_element_type=jnp.float32))
    dw_q = jnp.dot(normed.T, g_q, preferred_element_type=jnp.float32)
    dw_k = jnp.dot(normed.T, g_k, preferred_element_type=jnp.float32)
    dw_v = jnp.dot(normed.T, g_v, preferred_element_type=jnp.float32)
    d_hid, d_lnw = norm_vjp(d_normed)
    return (attn_out, d_hid.astype(jnp.bfloat16), d_lnw.astype(jnp.bfloat16), dw_q.astype(jnp.bfloat16),
            dw_k.astype(jnp.bfloat16), dw_v.astype(jnp.bfloat16), dw_o.astype(jnp.bfloat16))
```

```python
import functools
import math
import jax
import jax.numpy as jnp
from jax import lax
from jax.experimental import pallas as pl
from jax.experimental.pallas import tpu as pltpu
from jax.sharding import PartitionSpec as P

HEAD_DIM = 128
LN_EPS = 1e-5
ROPE_BASE = 10000.0
SCALE = HEAD_DIM ** -0.5
EXP2_SCALE = SCALE * math.log2(math.e)
BLOCK = 512
VMEM_LIMIT = 56 * 1024 * 1024
LAST = (((1,), (1,)), ((), ()))
PLAIN = (((1,), (0,)), ((), ()))


def norm_f32(hid_f32, weight_f32):
    mean_val = jnp.mean(hid_f32, axis=-1, keepdims=True)
    centered = hid_f32 - mean_val
    var_val = jnp.mean(centered * centered, axis=-1, keepdims=True)
    return centered * lax.rsqrt(var_val + LN_EPS) * weight_f32


def rope_tables(positions):
    inv_freq = ROPE_BASE ** (-jnp.arange(0, HEAD_DIM, 2, dtype=jnp.float32) / HEAD_DIM)
    angles = positions.astype(jnp.float32)[:, None] * inv_freq[None, :]
    cos_t, sin_t = jnp.cos(angles), jnp.sin(angles)
    cos_full = jnp.stack([cos_t, cos_t], axis=-1).reshape(-1, HEAD_DIM)
    sin_full = jnp.stack([-sin_t, sin_t], axis=-1).reshape(-1, HEAD_DIM)
    return cos_full, sin_full


def swap_pairs(x):
    lane = lax.broadcasted_iota(jnp.int32, x.shape, 1)
    up = pltpu.roll(x, HEAD_DIM - 1, 1)
    down = pltpu.roll(x, 1, 1)
    return jnp.where(lane % 2 == 0, up, down)


def dot_f32(a, b, dims):
    return lax.dot_general(a, b, dims, preferred_element_type=jnp.float32)


def proj_kernel(h_ref, wq_ref, wk_ref, wv_ref, cos_ref, sin_ref, q_ref, k_ref, v_ref, kt_ref, vt_ref):
    h = h_ref[...]
    cos_t, sin_t = cos_ref[...], sin_ref[...]
    q = dot_f32(h, wq_ref[...], PLAIN)
    k = dot_f32(h, wk_ref[...], PLAIN)
    v = dot_f32(h, wv_ref[...], PLAIN)
    for n in range(q.shape[1] // HEAD_DIM):
        cols = slice(n * HEAD_DIM, (n + 1) * HEAD_DIM)
        qn, kn, vn = q[:, cols], k[:, cols], v[:, cols]
        q_ref[:, cols] = (qn * cos_t + swap_pairs(qn) * sin_t).astype(jnp.bfloat16)
        kn = kn * cos_t + swap_pairs(kn) * sin_t
        k_ref[:, cols] = kn.astype(jnp.bfloat16)
        v_ref[:, cols] = vn.astype(jnp.bfloat16)
        kt_ref[cols, :] = kn.T.astype(jnp.bfloat16)
        vt_ref[cols, :] = vn.T.astype(jnp.bfloat16)


def project(h_all, w_q, w_k, w_v, cos_full, sin_full):
    rows, depth = h_all.shape
    cols = w_q.shape[1]
    tile = BLOCK
    row_spec = lambda width: pl.BlockSpec((tile, width), lambda i: (i, 0))
    full = pl.BlockSpec((depth, cols), lambda i: (0, 0))
    col_spec = pl.BlockSpec((cols, tile), lambda i: (0, i))
    out = jax.ShapeDtypeStruct((rows, cols), jnp.bfloat16)
    out_t = jax.ShapeDtypeStruct((cols, rows), jnp.bfloat16)
    return pl.pallas_call(
        proj_kernel, grid=(rows // tile,),
        in_specs=[row_spec(depth), full, full, full, row_spec(HEAD_DIM), row_spec(HEAD_DIM)],
        out_specs=[row_spec(cols)] * 3 + [col_spec] * 2,
        out_shape=[out] * 3 + [out_t] * 2,
        compiler_params=pltpu.CompilerParams(vmem_limit_bytes=VMEM_LIMIT),
        cost_estimate=pl.CostEstimate(flops=6 * rows * depth * cols, bytes_accessed=2 * rows * (depth + 5 * cols), transcendentals=0),
        name="project",
    )(h_all, w_q, w_k, w_v, cos_full, sin_full)


def causal(st, key_start, q_start):
    keys = lax.broadcasted_iota(jnp.int32, st.shape, 0) + key_start
    qs = lax.broadcasted_iota(jnp.int32, st.shape, 1) + q_start
    return jnp.where(keys <= qs, st, -jnp.inf)


def fwd_kernel(q_ref, k_ref, vt_ref, o_ref, ot_ref, lse_ref, acc_ref):
    i = pl.program_id(1)
    q = q_ref[...]
    acc_ref[...] = jnp.zeros_like(acc_ref)

    def step(j, carry, masked):
        m, l = carry
        start = pl.multiple_of(j * BLOCK, BLOCK)
        st = dot_f32(k_ref[pl.ds(start, BLOCK), :], q, LAST)
        if masked:
            st = causal(st, 0, 0)
        m_new = jnp.maximum(m, jnp.max(st, axis=0, keepdims=True))
        p = jnp.exp2((st - m_new) * EXP2_SCALE)
        alpha = jnp.exp2((m - m_new) * EXP2_SCALE)
        l = l * alpha + jnp.sum(p, axis=0, keepdims=True)
        acc_ref[...] = acc_ref[...] * alpha + dot_f32(vt_ref[:, pl.ds(start, BLOCK)], p.astype(jnp.bfloat16), PLAIN)
        return m_new, l

    init = (jnp.full((1, q.shape[0]), -jnp.inf, jnp.float32), jnp.zeros((1, q.shape[0]), jnp.float32))
    carry = lax.fori_loop(0, i, lambda j, c: step(j, c, False), init)
    m, l = step(i, carry, True)
    ot = acc_ref[...] / l
    ot_ref[...] = ot
    o_ref[...] = ot.T.astype(jnp.bfloat16)
    lse_ref[0] = m * EXP2_SCALE + jnp.log2(l)


def attn_forward(q, k, vt):
    rows, cols = q.shape
    heads = cols // HEAD_DIM
    blocks = rows // BLOCK
    flops = 2 * 2 * rows * rows * cols // 2
    return pl.pallas_call(
        fwd_kernel, grid=(heads, blocks),
        in_specs=[pl.BlockSpec((BLOCK, HEAD_DIM), lambda h, i: (i, h)),
                  pl.BlockSpec((rows, HEAD_DIM), lambda h, i: (0, h)),
                  pl.BlockSpec((HEAD_DIM, rows), lambda h, i: (h, 0))],
        out_specs=[pl.BlockSpec((BLOCK, HEAD_DIM), lambda h, i: (i, h)),
                   pl.BlockSpec((HEAD_DIM, BLOCK), lambda h, i: (h, i)),
                   pl.BlockSpec((1, 1, BLOCK), lambda h, i: (h, 0, i))],
        out_shape=[jax.ShapeDtypeStruct((rows, cols), jnp.bfloat16),
                   jax.ShapeDtypeStruct((cols, rows), jnp.float32),
                   jax.ShapeDtypeStruct((heads, 1, rows), jnp.float32)],
        scratch_shapes=[pltpu.VMEM((HEAD_DIM, BLOCK), jnp.float32)],
        compiler_params=pltpu.CompilerParams(vmem_limit_bytes=VMEM_LIMIT),
        cost_estimate=pl.CostEstimate(flops=2 * flops, bytes_accessed=10 * rows * cols, transcendentals=0),
        name="attn_fwd",
    )(q, k, vt)


def unrope(x, cos_t, sin_t):
    x = x.astype(jnp.bfloat16).astype(jnp.float32)
    return (x * cos_t - swap_pairs(x) * sin_t).astype(jnp.bfloat16)


def bwd_kernel(q_ref, do_ref, ot_ref, lse_ref, k_ref, v_ref, kt_ref, cos_ref, sin_ref,
               gq_ref, gk_ref, gv_ref, dk_acc, dv_acc, dqt_acc):
    i = pl.program_id(1)

    @pl.when(i == 0)
    def _():
        dk_acc[...] = jnp.zeros_like(dk_acc)
        dv_acc[...] = jnp.zeros_like(dv_acc)

    q = q_ref[...]
    do = do_ref[...]
    lse = lse_ref[0]
    row_dot = jnp.sum(do.astype(jnp.float32).T * ot_ref[...], axis=0, keepdims=True)
    dqt_acc[...] = jnp.zeros_like(dqt_acc)

    def step(j, masked):
        start = pl.multiple_of(j * BLOCK, BLOCK)
        rows = pl.ds(start, BLOCK)
        st = dot_f32(k_ref[rows, :], q, LAST)
        dpt = dot_f32(v_ref[rows, :], do, LAST)
        if masked:
            st = causal(st, 0, 0)
        p = jnp.exp2(st * EXP2_SCALE - lse)
        ds = (p * (dpt - row_dot) * SCALE).astype(jnp.bfloat16)
        dv_acc[rows, :] += dot_f32(p.astype(jnp.bfloat16), do, PLAIN)
        dk_acc[rows, :] += dot_f32(ds, q, PLAIN)
        dqt_acc[...] += dot_f32(kt_ref[:, rows], ds, PLAIN)

    lax.fori_loop(0, i, lambda j, c: (step(j, False), c)[1], 0)
    step(i, True)
    tile = pl.ds(pl.multiple_of(i * BLOCK, BLOCK), BLOCK)
    gq_ref[...] = unrope(dqt_acc[...].T, cos_ref[tile, :], sin_ref[tile, :])

    @pl.when(i == pl.num_programs(1) - 1)
    def _():
        def finish(j, c):
            rows = pl.ds(pl.multiple_of(j * BLOCK, BLOCK), BLOCK)
            gk_ref[rows, :] = unrope(dk_acc[rows, :], cos_ref[rows, :], sin_ref[rows, :])
            gv_ref[rows, :] = dv_acc[rows, :].astype(jnp.bfloat16)
            return c
        lax.fori_loop(0, dk_acc.shape[0] // BLOCK, finish, 0)


def attn_backward(q, do, ot, lse, k, v, kt, cos_full, sin_full):
    rows, cols = q.shape
    heads = cols // HEAD_DIM
    flops = 2 * rows * rows * cols // 2
    q_spec = pl.BlockSpec((BLOCK, HEAD_DIM), lambda h, i: (i, h))
    all_spec = pl.BlockSpec((rows, HEAD_DIM), lambda h, i: (0, h))
    table = pl.BlockSpec((rows, HEAD_DIM), lambda h, i: (0, 0))
    out = jax.ShapeDtypeStruct((rows, cols), jnp.bfloat16)
    return pl.pallas_call(
        bwd_kernel, grid=(heads, rows // BLOCK),
        in_specs=[q_spec, q_spec,
                  pl.BlockSpec((HEAD_DIM, BLOCK), lambda h, i: (h, i)),
                  pl.BlockSpec((1, 1, BLOCK), lambda h, i: (h, 0, i)),
                  all_spec, all_spec,
                  pl.BlockSpec((HEAD_DIM, rows), lambda h, i: (h, 0)),
                  table, table],
        out_specs=[q_spec, all_spec, all_spec],
        out_shape=[out] * 3,
        scratch_shapes=[pltpu.VMEM((rows, HEAD_DIM), jnp.float32),
                        pltpu.VMEM((rows, HEAD_DIM), jnp.float32),
                        pltpu.VMEM((HEAD_DIM, BLOCK), jnp.float32)],
        compiler_params=pltpu.CompilerParams(vmem_limit_bytes=VMEM_LIMIT),
        cost_estimate=pl.CostEstimate(flops=5 * flops, bytes_accessed=20 * rows * cols, transcendentals=0),
        name="attn_bwd",
    )(q, do, ot, lse, k, v, kt, cos_full, sin_full)


def solution(mesh):
    sp_size = mesh.shape['sp']
    row_spec = P(('dp', 'sp'), None)
    pos_spec = P(('dp', 'sp'))
    full_spec = P(None, None)
    grad_spec = P('dp', None)

    def local_step(hidden, positions, d_attn, ln_weight, w_q, w_k, w_v, w_o):
        me = lax.axis_index('sp')
        cols = w_q.shape[1] // sp_size
        normed32, norm_vjp = jax.vjp(norm_f32, hidden.astype(jnp.float32), ln_weight.astype(jnp.float32))
        normed = normed32.astype(jnp.bfloat16)
        pos_all = lax.all_gather(positions, 'sp', tiled=True)
        h_all = lax.all_gather(normed, 'sp', tiled=True)
        g_all = lax.all_gather(d_attn, 'sp', tiled=True)
        cos_full, sin_full = rope_tables(pos_all)
        mine = lambda w, axis: lax.dynamic_slice_in_dim(w, me * cols, cols, axis)
        wq_my, wk_my, wv_my, wo_my = mine(w_q, 1), mine(w_k, 1), mine(w_v, 1), mine(w_o, 0)
        q, k, v, kt, vt = project(h_all, wq_my, wk_my, wv_my, cos_full, sin_full)
        o, ot, lse = attn_forward(q, k, vt)
        o_tok = lax.all_to_all(o, 'sp', 0, 1, tiled=True)
        d_o = jnp.einsum('td,ed->te', g_all, wo_my, preferred_element_type=jnp.float32).astype(jnp.bfloat16)
        dwo_my = jnp.einsum('te,td->ed', o, g_all, preferred_element_type=jnp.float32).astype(jnp.bfloat16)
        gq, gk, gv = attn_backward(q, d_o, ot, lse, k, v, kt, cos_full, sin_full)
        dw_o = lax.all_gather(dwo_my, 'sp', tiled=True)
        to_tok = lambda x: lax.all_to_all(x, 'sp', 0, 1, tiled=True)
        gq_tok, gk_tok, gv_tok = to_tok(gq), to_tok(gk), to_tok(gv)
        wgrad = lambda x: jnp.einsum('td,te->de', h_all, x, preferred_element_type=jnp.float32).astype(jnp.bfloat16)
        gather = lambda x: lax.all_gather(x, 'sp', axis=1, tiled=True)
        dw_q, dw_k, dw_v = gather(wgrad(gq)), gather(wgrad(gk)), gather(wgrad(gv))
        attn_out = jnp.dot(o_tok, w_o, preferred_element_type=jnp.float32).astype(jnp.bfloat16)
        d_normed = (jnp.einsum('te,de->td', gq_tok, w_q, preferred_element_type=jnp.float32)
                    + jnp.einsum('te,de->td', gk_tok, w_k, preferred_element_type=jnp.float32)
                    + jnp.einsum('te,de->td', gv_tok, w_v, preferred_element_type=jnp.float32))
        d_hid, d_lnw = norm_vjp(d_normed)
        d_lnw = lax.psum(d_lnw, 'sp')
        return (attn_out, d_hid.astype(jnp.bfloat16), d_lnw.astype(jnp.bfloat16), dw_q, dw_k, dw_v, dw_o)

    return jax.shard_map(local_step, mesh=mesh,
                         in_specs=(row_spec, pos_spec, row_spec, P(None), full_spec, full_spec, full_spec, full_spec),
                         out_specs=(row_spec, row_spec, P('dp'), grad_spec, grad_spec, grad_spec, grad_spec),
                         check_vma=False)
```

```python
import math
import jax
import jax.numpy as jnp
from jax import lax
from jax.experimental import pallas as pl
from jax.experimental.pallas import tpu as pltpu
from jax.sharding import PartitionSpec as P

HEAD_DIM = 128
LN_EPS = 1e-5
ROPE_BASE = 10000.0
SCALE = HEAD_DIM ** -0.5
EXP2_SCALE = SCALE * math.log2(math.e)
BLOCK = 512
SUB = 256
VMEM_LIMIT = 56 * 1024 * 1024
LAST = (((1,), (1,)), ((), ()))
PLAIN = (((1,), (0,)), ((), ()))


def norm_f32(hid_f32, weight_f32):
    mean_val = jnp.mean(hid_f32, axis=-1, keepdims=True)
    centered = hid_f32 - mean_val
    var_val = jnp.mean(centered * centered, axis=-1, keepdims=True)
    return centered * lax.rsqrt(var_val + LN_EPS) * weight_f32


def ln_kernel(x_ref, w_ref, h_ref):
    h_ref[...] = norm_f32(x_ref[...].astype(jnp.float32), w_ref[...]).astype(jnp.bfloat16)


def layer_norm(x, ln_weight):
    rows, width = x.shape
    tile = math.gcd(rows, 128)
    spec = pl.BlockSpec((tile, width), lambda i: (i, 0))
    return pl.pallas_call(
        ln_kernel, grid=(rows // tile,),
        in_specs=[spec, pl.BlockSpec((1, width), lambda i: (0, 0))], out_specs=spec,
        out_shape=jax.ShapeDtypeStruct(x.shape, jnp.bfloat16),
        compiler_params=pltpu.CompilerParams(vmem_limit_bytes=VMEM_LIMIT),
        cost_estimate=pl.CostEstimate(flops=10 * rows * width, bytes_accessed=4 * rows * width, transcendentals=0),
        name="layer_norm",
    )(x, ln_weight)


def rope_tables(positions):
    inv_freq = ROPE_BASE ** (-jnp.arange(0, HEAD_DIM, 2, dtype=jnp.float32) / HEAD_DIM)
    angles = positions.astype(jnp.float32)[:, None] * inv_freq[None, :]
    cos_t, sin_t = jnp.cos(angles), jnp.sin(angles)
    cos_full = jnp.stack([cos_t, cos_t], axis=-1).reshape(-1, HEAD_DIM)
    sin_full = jnp.stack([-sin_t, sin_t], axis=-1).reshape(-1, HEAD_DIM)
    return cos_full, sin_full


def swap_pairs(x):
    lane = lax.broadcasted_iota(jnp.int32, x.shape, 1)
    up = pltpu.roll(x, HEAD_DIM - 1, 1)
    down = pltpu.roll(x, 1, 1)
    return jnp.where(lane % 2 == 0, up, down)


def dot_f32(a, b, dims):
    return lax.dot_general(a, b, dims, preferred_element_type=jnp.float32)


def proj_kernel(h_ref, wq_ref, wk_ref, wv_ref, cos_ref, sin_ref, q_ref, k_ref, v_ref, kt_ref, vt_ref):
    h = h_ref[...]
    cos_t, sin_t = cos_ref[...], sin_ref[...]
    q = dot_f32(h, wq_ref[...], PLAIN)
    k = dot_f32(h, wk_ref[...], PLAIN)
    v = dot_f32(h, wv_ref[...], PLAIN)
    for n in range(q.shape[1] // HEAD_DIM):
        cols = slice(n * HEAD_DIM, (n + 1) * HEAD_DIM)
        qn, kn, vn = q[:, cols], k[:, cols], v[:, cols]
        q_ref[:, cols] = (qn * cos_t + swap_pairs(qn) * sin_t).astype(jnp.bfloat16)
        kn = kn * cos_t + swap_pairs(kn) * sin_t
        k_ref[:, cols] = kn.astype(jnp.bfloat16)
        v_ref[:, cols] = vn.astype(jnp.bfloat16)
        kt_ref[cols, :] = kn.T.astype(jnp.bfloat16)
        vt_ref[cols, :] = vn.T.astype(jnp.bfloat16)


def project(h_all, w_q, w_k, w_v, cos_full, sin_full):
    rows, depth = h_all.shape
    cols = w_q.shape[1]
    tile = BLOCK
    row_spec = lambda width: pl.BlockSpec((tile, width), lambda i: (i, 0))
    full = pl.BlockSpec((depth, cols), lambda i: (0, 0))
    col_spec = pl.BlockSpec((cols, tile), lambda i: (0, i))
    out = jax.ShapeDtypeStruct((rows, cols), jnp.bfloat16)
    out_t = jax.ShapeDtypeStruct((cols, rows), jnp.bfloat16)
    return pl.pallas_call(
        proj_kernel, grid=(rows // tile,),
        in_specs=[row_spec(depth), full, full, full, row_spec(HEAD_DIM), row_spec(HEAD_DIM)],
        out_specs=[row_spec(cols)] * 3 + [col_spec] * 2,
        out_shape=[out] * 3 + [out_t] * 2,
        compiler_params=pltpu.CompilerParams(vmem_limit_bytes=VMEM_LIMIT),
        cost_estimate=pl.CostEstimate(flops=6 * rows * depth * cols, bytes_accessed=2 * rows * (depth + 5 * cols), transcendentals=0),
        name="project",
    )(h_all, w_q, w_k, w_v, cos_full, sin_full)


def causal(st, row0, col0):
    keys = lax.broadcasted_iota(jnp.int32, st.shape, 0) + row0
    qs = lax.broadcasted_iota(jnp.int32, st.shape, 1) + col0
    return jnp.where(keys <= qs, st, -jnp.inf)


def fwd_kernel(q_ref, k_ref, vt_ref, o_ref, ot_ref, lse_ref, acc_ref, m_ref, l_ref):
    i = pl.program_id(1)
    rows = q_ref.shape[0]
    acc_ref[...] = jnp.zeros_like(acc_ref)
    m_ref[...] = jnp.full_like(m_ref, -jnp.inf)
    l_ref[...] = jnp.zeros_like(l_ref)

    def step(j, diagonal):
        start = pl.multiple_of(j * rows, rows)

        def scores(a):
            keys = a + SUB if diagonal else rows
            st = dot_f32(k_ref[pl.ds(start, keys), :], q_ref[a:a + SUB, :], LAST)
            return causal(st, 0, a) if diagonal else st

        def update(a, st):
            cols = slice(a, a + SUB)
            m = m_ref[:, cols]
            m_new = jnp.maximum(m, jnp.max(st, axis=0, keepdims=True))
            p = jnp.exp2((st - m_new) * EXP2_SCALE)
            alpha = jnp.exp2((m - m_new) * EXP2_SCALE)
            m_ref[:, cols] = m_new
            l_ref[:, cols] = l_ref[:, cols] * alpha + jnp.sum(p, axis=0, keepdims=True)
            pv = dot_f32(vt_ref[:, pl.ds(start, st.shape[0])], p.astype(jnp.bfloat16), PLAIN)
            acc_ref[:, cols] = acc_ref[:, cols] * alpha + pv

        st = scores(0)
        for a in range(0, rows, SUB):
            ahead = scores(a + SUB) if a + SUB < rows else None
            update(a, st)
            st = ahead

    lax.fori_loop(0, i, lambda j, c: (step(j, False), c)[1], 0)
    step(i, True)
    ot = acc_ref[...] / l_ref[...]
    ot_ref[...] = ot
    o_ref[...] = ot.T.astype(jnp.bfloat16)
    lse_ref[0] = m_ref[...] * EXP2_SCALE + jnp.log2(l_ref[...])


def attn_forward(q, k, vt, block):
    rows, cols = q.shape
    heads = cols // HEAD_DIM
    flops = 2 * 2 * rows * rows * cols // 2
    return pl.pallas_call(
        fwd_kernel, grid=(heads, rows // block),
        in_specs=[pl.BlockSpec((block, HEAD_DIM), lambda h, i: (i, h)),
                  pl.BlockSpec((rows, HEAD_DIM), lambda h, i: (0, h)),
                  pl.BlockSpec((HEAD_DIM, rows), lambda h, i: (h, 0))],
        out_specs=[pl.BlockSpec((block, HEAD_DIM), lambda h, i: (i, h)),
                   pl.BlockSpec((HEAD_DIM, block), lambda h, i: (h, i)),
                   pl.BlockSpec((1, 1, block), lambda h, i: (h, 0, i))],
        out_shape=[jax.ShapeDtypeStruct((rows, cols), jnp.bfloat16),
                   jax.ShapeDtypeStruct((cols, rows), jnp.float32),
                   jax.ShapeDtypeStruct((heads, 1, rows), jnp.float32)],
        scratch_shapes=[pltpu.VMEM((HEAD_DIM, block), jnp.float32),
                        pltpu.VMEM((1, block), jnp.float32),
                        pltpu.VMEM((1, block), jnp.float32)],
        compiler_params=pltpu.CompilerParams(vmem_limit_bytes=VMEM_LIMIT),
        cost_estimate=pl.CostEstimate(flops=2 * flops, bytes_accessed=10 * rows * cols, transcendentals=0),
        name="attn_fwd",
    )(q, k, vt)


def unrope(x, cos_t, sin_t):
    x = x.astype(jnp.bfloat16).astype(jnp.float32)
    return (x * cos_t - swap_pairs(x) * sin_t).astype(jnp.bfloat16)


def bwd_kernel(q_ref, do_ref, ot_ref, lse_ref, k_ref, v_ref, kt_ref, cos_ref, sin_ref,
               g_ref, dk_acc, dv_acc, dqt_acc):
    i = pl.program_id(0)
    rows = q_ref.shape[0]

    @pl.when(i == 0)
    def _():
        dk_acc[...] = jnp.zeros_like(dk_acc)
        dv_acc[...] = jnp.zeros_like(dv_acc)

    lse = lse_ref[0]
    row_dot = jnp.sum(do_ref[...].astype(jnp.float32).T * ot_ref[...], axis=0, keepdims=True)
    dqt_acc[...] = jnp.zeros_like(dqt_acc)

    def step(j, diagonal):
        start = pl.multiple_of(j * rows, rows)

        def scores(b):
            first = b if diagonal else 0
            keys = pl.ds(start + b, SUB)
            st = dot_f32(k_ref[keys, :], q_ref[first:, :], LAST)
            dpt = dot_f32(v_ref[keys, :], do_ref[first:, :], LAST)
            return st, dpt

        def update(b, st, dpt):
            first = b if diagonal else 0
            keys = pl.ds(start + b, SUB)
            if diagonal:
                st = causal(st, b, first)
            p = jnp.exp2(st * EXP2_SCALE - lse[:, first:])
            ds = (p * (dpt - row_dot[:, first:]) * SCALE).astype(jnp.bfloat16)
            dv_acc[keys, :] += dot_f32(p.astype(jnp.bfloat16), do_ref[first:, :], PLAIN)
            dk_acc[keys, :] += dot_f32(ds, q_ref[first:, :], PLAIN)
            dqt_acc[:, first:] += dot_f32(kt_ref[:, keys], ds, PLAIN)

        now = scores(0)
        for b in range(0, rows, SUB):
            ahead = scores(b + SUB) if b + SUB < rows else None
            update(b, *now)
            now = ahead

    lax.fori_loop(0, i, lambda j, c: (step(j, False), c)[1], 0)
    step(i, True)
    tile = pl.ds(pl.multiple_of(i * rows, rows), rows)
    g_ref[tile, :HEAD_DIM] = unrope(dqt_acc[...].T, cos_ref[tile, :], sin_ref[tile, :])

    @pl.when(i == pl.num_programs(0) - 1)
    def _():
        def finish(j, c):
            part = pl.ds(pl.multiple_of(j * rows, rows), rows)
            g_ref[part, HEAD_DIM:2 * HEAD_DIM] = unrope(dk_acc[part, :], cos_ref[part, :], sin_ref[part, :])
            g_ref[part, 2 * HEAD_DIM:] = dv_acc[part, :].astype(jnp.bfloat16)
            return c

        lax.fori_loop(0, dk_acc.shape[0] // rows, finish, 0)


def attn_backward(q, do, ot, lse, k, v, kt, cos_full, sin_full, block, head):
    rows = q.shape[0]
    flops = 2 * rows * rows * HEAD_DIM // 2
    q_spec = pl.BlockSpec((block, HEAD_DIM), lambda i: (i, head))
    all_spec = pl.BlockSpec((rows, HEAD_DIM), lambda i: (0, head))
    table = pl.BlockSpec((rows, HEAD_DIM), lambda i: (0, 0))
    return pl.pallas_call(
        bwd_kernel, grid=(rows // block,),
        in_specs=[q_spec, q_spec,
                  pl.BlockSpec((HEAD_DIM, block), lambda i: (head, i)),
                  pl.BlockSpec((1, 1, block), lambda i: (head, 0, i)),
                  all_spec, all_spec,
                  pl.BlockSpec((HEAD_DIM, rows), lambda i: (head, 0)),
                  table, table],
        out_specs=pl.BlockSpec((rows, 3 * HEAD_DIM), lambda i: (0, 0)),
        out_shape=jax.ShapeDtypeStruct((rows, 3 * HEAD_DIM), jnp.bfloat16),
        scratch_shapes=[pltpu.VMEM((rows, HEAD_DIM), jnp.float32),
                        pltpu.VMEM((rows, HEAD_DIM), jnp.float32),
                        pltpu.VMEM((HEAD_DIM, block), jnp.float32)],
        compiler_params=pltpu.CompilerParams(vmem_limit_bytes=VMEM_LIMIT),
        cost_estimate=pl.CostEstimate(flops=2 * 5 * flops, bytes_accessed=20 * rows * HEAD_DIM, transcendentals=0),
        name="attn_bwd",
    )(q, do, ot, lse, k, v, kt, cos_full, sin_full)


def out_kernel(o_ref, w_ref, slab_ref, a_ref, dwo_ref, acc_ref):
    d = pl.program_id(0)
    dwo_ref[...] = slab_ref[...]

    @pl.when(d == 0)
    def _():
        acc_ref[...] = jnp.zeros_like(acc_ref)

    acc_ref[...] += dot_f32(o_ref[0], w_ref[...], PLAIN)

    @pl.when(d == pl.num_programs(0) - 1)
    def _():
        a_ref[...] = acc_ref[...].astype(jnp.bfloat16)


def out_project(o_chunks, w_o, dwo_slab):
    n, rows, cols = o_chunks.shape
    width = w_o.shape[1]
    return pl.pallas_call(
        out_kernel, grid=(n,),
        in_specs=[pl.BlockSpec((1, rows, cols), lambda d: (d, 0, 0)),
                  pl.BlockSpec((cols, width), lambda d: (d, 0)),
                  pl.BlockSpec((cols, width), lambda d: (d, 0))],
        out_specs=[pl.BlockSpec((rows, width), lambda d: (0, 0)),
                   pl.BlockSpec((cols, width), lambda d: (d, 0))],
        out_shape=[jax.ShapeDtypeStruct((rows, width), jnp.bfloat16),
                   jax.ShapeDtypeStruct(w_o.shape, jnp.bfloat16)],
        scratch_shapes=[pltpu.VMEM((rows, width), jnp.float32)],
        compiler_params=pltpu.CompilerParams(vmem_limit_bytes=VMEM_LIMIT),
        cost_estimate=pl.CostEstimate(flops=2 * n * rows * cols * width, bytes_accessed=2 * n * cols * (rows + width), transcendentals=0),
        name="out_project",
    )(o_chunks, w_o, dwo_slab)


def tail_kernel(ga_ref, gb_ref, wq_ref, wk_ref, wv_ref, x_ref, lnw_ref, dx_ref, dlnw_ref, acc_ref):
    d = pl.program_id(0)

    @pl.when(d == 0)
    def _():
        acc_ref[...] = jnp.zeros_like(acc_ref)

    for part, w_ref in enumerate((wq_ref, wk_ref, wv_ref)):
        cols = slice(part * HEAD_DIM, (part + 1) * HEAD_DIM)
        both = jnp.concatenate([ga_ref[0, :, cols], gb_ref[0, :, cols]], axis=1)
        acc_ref[...] += dot_f32(both, w_ref[...], LAST)

    @pl.when(d == pl.num_programs(0) - 1)
    def _():
        dlnw_ref[...] = jnp.zeros_like(dlnw_ref)
        lnw = lnw_ref[...]
        step = 64

        def rows_step(t, c):
            rows = pl.ds(pl.multiple_of(t * step, step), step)
            x = x_ref[rows, :].astype(jnp.float32)
            dh = acc_ref[rows, :]
            centered = x - jnp.mean(x, axis=-1, keepdims=True)
            rstd = lax.rsqrt(jnp.mean(centered * centered, axis=-1, keepdims=True) + LN_EPS)
            xhat = centered * rstd
            dlnw_ref[...] += jnp.sum(dh * xhat, axis=0, keepdims=True)
            dxhat = dh * lnw
            dx = rstd * (dxhat - jnp.mean(dxhat, axis=-1, keepdims=True) - xhat * jnp.mean(dxhat * xhat, axis=-1, keepdims=True))
            dx_ref[rows, :] = dx.astype(jnp.bfloat16)
            return c

        lax.fori_loop(0, x_ref.shape[0] // step, rows_step, 0)


def tail(ga, gb, w_q, w_k, w_v, hidden, ln_weight):
    n, rows, cols = ga.shape
    width = hidden.shape[1]
    g_spec = pl.BlockSpec((1, rows, cols), lambda d: (d, 0, 0))
    w_spec = pl.BlockSpec((width, 2 * HEAD_DIM), lambda d: (0, d))
    whole = pl.BlockSpec((rows, width), lambda d: (0, 0))
    row = pl.BlockSpec((1, width), lambda d: (0, 0))
    return pl.pallas_call(
        tail_kernel, grid=(n,),
        in_specs=[g_spec, g_spec, w_spec, w_spec, w_spec, whole, row],
        out_specs=[whole, row],
        out_shape=[jax.ShapeDtypeStruct((rows, width), jnp.bfloat16), jax.ShapeDtypeStruct((1, width), jnp.float32)],
        scratch_shapes=[pltpu.VMEM((rows, width), jnp.float32)],
        compiler_params=pltpu.CompilerParams(vmem_limit_bytes=VMEM_LIMIT),
        cost_estimate=pl.CostEstimate(flops=4 * n * rows * cols * width, bytes_accessed=4 * n * cols * (rows + width), transcendentals=0),
        name="tail",
    )(ga, gb, w_q, w_k, w_v, hidden, ln_weight)


def assemble_kernel(slab_ref, *refs):
    for part, out in enumerate(refs[-3:]):
        out[...] = slab_ref[0, :, part * HEAD_DIM:(part + 1) * HEAD_DIM]


def assemble(slab, head, heads, into=()):
    n, rows, cols = slab.shape
    out_spec = pl.BlockSpec((rows, HEAD_DIM), lambda d: (0, heads * d + head))
    out = jax.ShapeDtypeStruct((rows, n * heads * HEAD_DIM), jnp.bfloat16)
    return pl.pallas_call(
        assemble_kernel, grid=(n,),
        in_specs=[pl.BlockSpec((1, rows, cols), lambda d: (d, 0, 0))] + [pl.BlockSpec(memory_space=pl.ANY)] * len(into),
        out_specs=[out_spec] * 3, out_shape=[out] * 3,
        input_output_aliases={1 + i: i for i in range(len(into))},
        compiler_params=pltpu.CompilerParams(vmem_limit_bytes=VMEM_LIMIT),
        cost_estimate=pl.CostEstimate(flops=rows * n * cols * 64, bytes_accessed=4 * n * rows * cols, transcendentals=0),
        name="assemble",
    )(slab, *into)


def solution(mesh):
    sp_size = mesh.shape['sp']
    row_spec = P(('dp', 'sp'), None)
    pos_spec = P(('dp', 'sp'))
    full_spec = P(None, None)
    grad_spec = P('dp', None)

    def layer(hidden, positions, d_attn, ln_weight, w_q, w_k, w_v, w_o):
        me = lax.axis_index('sp')
        block = hidden.shape[0]
        cols = w_q.shape[1] // sp_size
        lnw32 = ln_weight.astype(jnp.float32)
        normed = layer_norm(hidden, lnw32[None])
        pos_all = lax.all_gather(positions, 'sp', tiled=True)
        h_all = lax.all_gather(normed, 'sp', tiled=True)
        g_all = lax.all_gather(d_attn, 'sp', tiled=True)
        cos_full, sin_full = rope_tables(pos_all)
        mine = lambda w, axis: lax.dynamic_slice_in_dim(w, me * cols, cols, axis)
        wq_my, wk_my, wv_my, wo_my = mine(w_q, 1), mine(w_k, 1), mine(w_v, 1), mine(w_o, 0)
        q, k, v, kt, vt = project(h_all, wq_my, wk_my, wv_my, cos_full, sin_full)

        def exchange(x):
            return lax.all_to_all(x.reshape(sp_size, block, x.shape[1]), 'sp', 0, 0)

        o, ot, lse = attn_forward(q, k, vt, block)
        o_chunks = exchange(o)
        d_o = jnp.einsum('td,ed->te', g_all, wo_my, preferred_element_type=jnp.float32).astype(jnp.bfloat16)

        def back(q, head):
            return attn_backward(q, d_o, ot, lse, k, v, kt, cos_full, sin_full, block, head)

        def wgrad(x):
            return jnp.einsum('td,te->de', h_all, x, preferred_element_type=jnp.float32).astype(jnp.bfloat16)

        dwo_my = jnp.einsum('te,td->ed', o, g_all, preferred_element_type=jnp.float32).astype(jnp.bfloat16)
        q_0, dwo_my = lax.optimization_barrier((q, dwo_my))
        dwo_slab = lax.all_gather(dwo_my, 'sp', tiled=True)
        g_a = back(q_0, 0)
        sent_a, o_chunks = lax.optimization_barrier((g_a, o_chunks))
        ga_tok = exchange(sent_a)
        q_1, part_a = lax.optimization_barrier((q, wgrad(g_a)))
        slab_a = lax.all_gather(part_a, 'sp')
        g_b = back(q_1, 1)
        sent_b, ga_tok = lax.optimization_barrier((g_b, ga_tok))
        gb_tok = exchange(sent_b)
        slab_b = lax.all_gather(wgrad(g_b), 'sp')
        attn_out, dw_o = out_project(o_chunks, w_o, dwo_slab)
        d_hid, d_lnw = tail(ga_tok, gb_tok, w_q, w_k, w_v, hidden, lnw32[None])
        d_lnw = lax.psum(d_lnw[0], 'sp').astype(jnp.bfloat16)
        half = assemble(slab_a, 0, 2)
        half, d_hid, attn_out, slab_b = lax.optimization_barrier((half, d_hid, attn_out, slab_b))
        dw_q, dw_k, dw_v = assemble(slab_b, 1, 2, half)
        return attn_out, d_hid, d_lnw, dw_q, dw_k, dw_v, dw_o

    return jax.shard_map(layer, mesh=mesh,
                         in_specs=(row_spec, pos_spec, row_spec, P(None), full_spec, full_spec, full_spec, full_spec),
                         out_specs=(row_spec, row_spec, P('dp'), grad_spec, grad_spec, grad_spec, grad_spec),
                         check_vma=False)
```

```python
import math
import jax
import jax.numpy as jnp
from jax import lax
from jax.experimental import pallas as pl
from jax.experimental.pallas import tpu as pltpu
from jax.sharding import PartitionSpec as P

HEAD_DIM = 128
LN_EPS = 1e-5
ROPE_BASE = 10000.0
SCALE = HEAD_DIM ** -0.5
EXP2_SCALE = SCALE * math.log2(math.e)
BLOCK = 512
SUB = 256
VMEM_LIMIT = 56 * 1024 * 1024
LAST = (((1,), (1,)), ((), ()))
PLAIN = (((1,), (0,)), ((), ()))


def norm_f32(hid_f32, weight_f32):
    mean_val = jnp.mean(hid_f32, axis=-1, keepdims=True)
    centered = hid_f32 - mean_val
    var_val = jnp.mean(centered * centered, axis=-1, keepdims=True)
    return centered * lax.rsqrt(var_val + LN_EPS) * weight_f32


def ln_kernel(x_ref, w_ref, h_ref):
    h_ref[...] = norm_f32(x_ref[...].astype(jnp.float32), w_ref[...]).astype(jnp.bfloat16)


def layer_norm(x, ln_weight):
    rows, width = x.shape
    tile = math.gcd(rows, 128)
    spec = pl.BlockSpec((tile, width), lambda i: (i, 0))
    return pl.pallas_call(
        ln_kernel, grid=(rows // tile,),
        in_specs=[spec, pl.BlockSpec((1, width), lambda i: (0, 0))], out_specs=spec,
        out_shape=jax.ShapeDtypeStruct(x.shape, jnp.bfloat16),
        compiler_params=pltpu.CompilerParams(vmem_limit_bytes=VMEM_LIMIT),
        cost_estimate=pl.CostEstimate(flops=10 * rows * width, bytes_accessed=4 * rows * width, transcendentals=0),
        name="layer_norm",
    )(x, ln_weight)


def rope_tables(positions):
    inv_freq = ROPE_BASE ** (-jnp.arange(0, HEAD_DIM, 2, dtype=jnp.float32) / HEAD_DIM)
    angles = positions.astype(jnp.float32)[:, None] * inv_freq[None, :]
    cos_t, sin_t = jnp.cos(angles), jnp.sin(angles)
    cos_full = jnp.stack([cos_t, cos_t], axis=-1).reshape(-1, HEAD_DIM)
    sin_full = jnp.stack([-sin_t, sin_t], axis=-1).reshape(-1, HEAD_DIM)
    return cos_full, sin_full


def swap_pairs(x):
    lane = lax.broadcasted_iota(jnp.int32, x.shape, 1)
    up = pltpu.roll(x, HEAD_DIM - 1, 1)
    down = pltpu.roll(x, 1, 1)
    return jnp.where(lane % 2 == 0, up, down)


def dot_f32(a, b, dims):
    return lax.dot_general(a, b, dims, preferred_element_type=jnp.float32)


def proj_kernel(h_ref, wq_ref, wk_ref, wv_ref, cos_ref, sin_ref, q_ref, k_ref, v_ref, kt_ref, vt_ref):
    h = h_ref[...]
    cos_t, sin_t = cos_ref[...], sin_ref[...]
    q = dot_f32(h, wq_ref[...], PLAIN)
    k = dot_f32(h, wk_ref[...], PLAIN)
    v = dot_f32(h, wv_ref[...], PLAIN)
    for n in range(q.shape[1] // HEAD_DIM):
        cols = slice(n * HEAD_DIM, (n + 1) * HEAD_DIM)
        qn, kn, vn = q[:, cols], k[:, cols], v[:, cols]
        q_ref[:, cols] = (qn * cos_t + swap_pairs(qn) * sin_t).astype(jnp.bfloat16)
        kn = kn * cos_t + swap_pairs(kn) * sin_t
        k_ref[:, cols] = kn.astype(jnp.bfloat16)
        v_ref[:, cols] = vn.astype(jnp.bfloat16)
        kt_ref[cols, :] = kn.T.astype(jnp.bfloat16)
        vt_ref[cols, :] = vn.T.astype(jnp.bfloat16)


def project(h_all, w_q, w_k, w_v, cos_full, sin_full):
    rows, depth = h_all.shape
    cols = w_q.shape[1]
    tile = BLOCK
    row_spec = lambda width: pl.BlockSpec((tile, width), lambda i: (i, 0))
    full = pl.BlockSpec((depth, cols), lambda i: (0, 0))
    col_spec = pl.BlockSpec((cols, tile), lambda i: (0, i))
    out = jax.ShapeDtypeStruct((rows, cols), jnp.bfloat16)
    out_t = jax.ShapeDtypeStruct((cols, rows), jnp.bfloat16)
    return pl.pallas_call(
        proj_kernel, grid=(rows // tile,),
        in_specs=[row_spec(depth), full, full, full, row_spec(HEAD_DIM), row_spec(HEAD_DIM)],
        out_specs=[row_spec(cols)] * 3 + [col_spec] * 2,
        out_shape=[out] * 3 + [out_t] * 2,
        compiler_params=pltpu.CompilerParams(vmem_limit_bytes=VMEM_LIMIT),
        cost_estimate=pl.CostEstimate(flops=6 * rows * depth * cols, bytes_accessed=2 * rows * (depth + 5 * cols), transcendentals=0),
        name="project",
    )(h_all, w_q, w_k, w_v, cos_full, sin_full)


def causal(st, row0, col0):
    keys = lax.broadcasted_iota(jnp.int32, st.shape, 0) + row0
    qs = lax.broadcasted_iota(jnp.int32, st.shape, 1) + col0
    return jnp.where(keys <= qs, st, -jnp.inf)


def fwd_kernel(q_ref, k_ref, vt_ref, o_ref, ot_ref, lse_ref, acc_ref, m_ref, l_ref):
    i = pl.program_id(1)
    rows = q_ref.shape[0]
    acc_ref[...] = jnp.zeros_like(acc_ref)
    m_ref[...] = jnp.full_like(m_ref, -jnp.inf)
    l_ref[...] = jnp.zeros_like(l_ref)

    def step(j, diagonal):
        start = pl.multiple_of(j * rows, rows)

        def scores(a):
            keys = a + SUB if diagonal else rows
            st = dot_f32(k_ref[pl.ds(start, keys), :], q_ref[a:a + SUB, :], LAST)
            return causal(st, 0, a) if diagonal else st

        def update(a, st):
            cols = slice(a, a + SUB)
            m = m_ref[:, cols]
            m_new = jnp.maximum(m, jnp.max(st, axis=0, keepdims=True))
            p = jnp.exp2((st - m_new) * EXP2_SCALE)
            alpha = jnp.exp2((m - m_new) * EXP2_SCALE)
            m_ref[:, cols] = m_new
            l_ref[:, cols] = l_ref[:, cols] * alpha + jnp.sum(p, axis=0, keepdims=True)
            pv = dot_f32(vt_ref[:, pl.ds(start, st.shape[0])], p.astype(jnp.bfloat16), PLAIN)
            acc_ref[:, cols] = acc_ref[:, cols] * alpha + pv

        st = scores(0)
        for a in range(0, rows, SUB):
            ahead = scores(a + SUB) if a + SUB < rows else None
            update(a, st)
            st = ahead

    lax.fori_loop(0, i, lambda j, c: (step(j, False), c)[1], 0)
    step(i, True)
    ot = acc_ref[...] / l_ref[...]
    ot_ref[...] = ot
    o_ref[...] = ot.T.astype(jnp.bfloat16)
    lse_ref[0] = m_ref[...] * EXP2_SCALE + jnp.log2(l_ref[...])


def attn_forward(q, k, vt, block):
    rows, cols = q.shape
    heads = cols // HEAD_DIM
    flops = 2 * 2 * rows * rows * cols // 2
    return pl.pallas_call(
        fwd_kernel, grid=(heads, rows // block),
        in_specs=[pl.BlockSpec((block, HEAD_DIM), lambda h, i: (i, h)),
                  pl.BlockSpec((rows, HEAD_DIM), lambda h, i: (0, h)),
                  pl.BlockSpec((HEAD_DIM, rows), lambda h, i: (h, 0))],
        out_specs=[pl.BlockSpec((block, HEAD_DIM), lambda h, i: (i, h)),
                   pl.BlockSpec((HEAD_DIM, block), lambda h, i: (h, i)),
                   pl.BlockSpec((1, 1, block), lambda h, i: (h, 0, i))],
        out_shape=[jax.ShapeDtypeStruct((rows, cols), jnp.bfloat16),
                   jax.ShapeDtypeStruct((cols, rows), jnp.float32),
                   jax.ShapeDtypeStruct((heads, 1, rows), jnp.float32)],
        scratch_shapes=[pltpu.VMEM((HEAD_DIM, block), jnp.float32),
                        pltpu.VMEM((1, block), jnp.float32),
                        pltpu.VMEM((1, block), jnp.float32)],
        compiler_params=pltpu.CompilerParams(vmem_limit_bytes=VMEM_LIMIT),
        cost_estimate=pl.CostEstimate(flops=2 * flops, bytes_accessed=10 * rows * cols, transcendentals=0),
        name="attn_fwd",
    )(q, k, vt)


def unrope(x, cos_t, sin_t):
    x = x.astype(jnp.bfloat16).astype(jnp.float32)
    return (x * cos_t - swap_pairs(x) * sin_t).astype(jnp.bfloat16)


def bwd_kernel(q_ref, do_ref, ot_ref, lse_ref, k_ref, v_ref, kt_ref, cos_ref, sin_ref,
               g_ref, dk_acc, dv_acc, dqt_acc):
    i = pl.program_id(0)
    rows = q_ref.shape[0]

    @pl.when(i == 0)
    def _():
        dk_acc[...] = jnp.zeros_like(dk_acc)
        dv_acc[...] = jnp.zeros_like(dv_acc)

    lse = lse_ref[0]
    row_dot = jnp.sum(do_ref[...].astype(jnp.float32).T * ot_ref[...], axis=0, keepdims=True)
    dqt_acc[...] = jnp.zeros_like(dqt_acc)

    def step(j, diagonal):
        start = pl.multiple_of(j * rows, rows)

        def scores(b):
            first = b if diagonal else 0
            keys = pl.ds(start + b, SUB)
            st = dot_f32(k_ref[keys, :], q_ref[first:, :], LAST)
            dpt = dot_f32(v_ref[keys, :], do_ref[first:, :], LAST)
            return st, dpt

        def update(b, st, dpt):
            first = b if diagonal else 0
            keys = pl.ds(start + b, SUB)
            if diagonal:
                st = causal(st, b, first)
            p = jnp.exp2(st * EXP2_SCALE - lse[:, first:])
            ds = (p * (dpt - row_dot[:, first:]) * SCALE).astype(jnp.bfloat16)
            dv_acc[keys, :] += dot_f32(p.astype(jnp.bfloat16), do_ref[first:, :], PLAIN)
            dk_acc[keys, :] += dot_f32(ds, q_ref[first:, :], PLAIN)
            dqt_acc[:, first:] += dot_f32(kt_ref[:, keys], ds, PLAIN)

        now = scores(0)
        for b in range(0, rows, SUB):
            ahead = scores(b + SUB) if b + SUB < rows else None
            update(b, *now)
            now = ahead

    lax.fori_loop(0, i, lambda j, c: (step(j, False), c)[1], 0)
    step(i, True)
    tile = pl.ds(pl.multiple_of(i * rows, rows), rows)
    g_ref[tile, :HEAD_DIM] = unrope(dqt_acc[...].T, cos_ref[tile, :], sin_ref[tile, :])

    @pl.when(i == pl.num_programs(0) - 1)
    def _():
        def finish(j, c):
            part = pl.ds(pl.multiple_of(j * rows, rows), rows)
            g_ref[part, HEAD_DIM:2 * HEAD_DIM] = unrope(dk_acc[part, :], cos_ref[part, :], sin_ref[part, :])
            g_ref[part, 2 * HEAD_DIM:] = dv_acc[part, :].astype(jnp.bfloat16)
            return c

        lax.fori_loop(0, dk_acc.shape[0] // rows, finish, 0)


def attn_backward(q, do, ot, lse, k, v, kt, cos_full, sin_full, block, head):
    rows = q.shape[0]
    flops = 2 * rows * rows * HEAD_DIM // 2
    q_spec = pl.BlockSpec((block, HEAD_DIM), lambda i: (i, head))
    all_spec = pl.BlockSpec((rows, HEAD_DIM), lambda i: (0, head))
    table = pl.BlockSpec((rows, HEAD_DIM), lambda i: (0, 0))
    return pl.pallas_call(
        bwd_kernel, grid=(rows // block,),
        in_specs=[q_spec, q_spec,
                  pl.BlockSpec((HEAD_DIM, block), lambda i: (head, i)),
                  pl.BlockSpec((1, 1, block), lambda i: (head, 0, i)),
                  all_spec, all_spec,
                  pl.BlockSpec((HEAD_DIM, rows), lambda i: (head, 0)),
                  table, table],
        out_specs=pl.BlockSpec((rows, 3 * HEAD_DIM), lambda i: (0, 0)),
        out_shape=jax.ShapeDtypeStruct((rows, 3 * HEAD_DIM), jnp.bfloat16),
        scratch_shapes=[pltpu.VMEM((rows, HEAD_DIM), jnp.float32),
                        pltpu.VMEM((rows, HEAD_DIM), jnp.float32),
                        pltpu.VMEM((HEAD_DIM, block), jnp.float32)],
        compiler_params=pltpu.CompilerParams(vmem_limit_bytes=VMEM_LIMIT),
        cost_estimate=pl.CostEstimate(flops=2 * 5 * flops, bytes_accessed=20 * rows * HEAD_DIM, transcendentals=0),
        name="attn_bwd",
    )(q, do, ot, lse, k, v, kt, cos_full, sin_full)


def cot_kernel(g_ref, w_ref, ot_ref, do_ref, dw_ref, acc_ref):
    t = pl.program_id(0)

    @pl.when(t == 0)
    def _():
        acc_ref[...] = jnp.zeros_like(acc_ref)

    g = g_ref[...]
    do_ref[...] = dot_f32(g, w_ref[...], LAST).astype(jnp.bfloat16)
    acc_ref[...] += dot_f32(ot_ref[...].astype(jnp.bfloat16), g, PLAIN)

    @pl.when(t == pl.num_programs(0) - 1)
    def _():
        dw_ref[...] = acc_ref[...].astype(jnp.bfloat16)


def cotangents(g_all, wo_my, ot, block):
    rows, width = g_all.shape
    cols = wo_my.shape[0]
    slab = pl.BlockSpec((cols, width), lambda t: (0, 0))
    return pl.pallas_call(
        cot_kernel, grid=(rows // block,),
        in_specs=[pl.BlockSpec((block, width), lambda t: (t, 0)), slab, pl.BlockSpec((cols, block), lambda t: (0, t))],
        out_specs=[pl.BlockSpec((block, cols), lambda t: (t, 0)), slab],
        out_shape=[jax.ShapeDtypeStruct((rows, cols), jnp.bfloat16), jax.ShapeDtypeStruct((cols, width), jnp.bfloat16)],
        scratch_shapes=[pltpu.VMEM((cols, width), jnp.float32)],
        compiler_params=pltpu.CompilerParams(vmem_limit_bytes=VMEM_LIMIT),
        cost_estimate=pl.CostEstimate(flops=4 * rows * cols * width, bytes_accessed=2 * rows * (width + 3 * cols), transcendentals=0),
        name="cotangents",
    )(g_all, wo_my, ot)


def out_kernel(o_ref, w_ref, slab_ref, a_ref, dwo_ref, acc_ref):
    d = pl.program_id(0)
    dwo_ref[...] = slab_ref[...]

    @pl.when(d == 0)
    def _():
        acc_ref[...] = jnp.zeros_like(acc_ref)

    acc_ref[...] += dot_f32(o_ref[0], w_ref[...], PLAIN)

    @pl.when(d == pl.num_programs(0) - 1)
    def _():
        a_ref[...] = acc_ref[...].astype(jnp.bfloat16)


def out_project(o_chunks, w_o, dwo_slab):
    n, rows, cols = o_chunks.shape
    width = w_o.shape[1]
    return pl.pallas_call(
        out_kernel, grid=(n,),
        in_specs=[pl.BlockSpec((1, rows, cols), lambda d: (d, 0, 0)),
                  pl.BlockSpec((cols, width), lambda d: (d, 0)),
                  pl.BlockSpec((cols, width), lambda d: (d, 0))],
        out_specs=[pl.BlockSpec((rows, width), lambda d: (0, 0)),
                   pl.BlockSpec((cols, width), lambda d: (d, 0))],
        out_shape=[jax.ShapeDtypeStruct((rows, width), jnp.bfloat16),
                   jax.ShapeDtypeStruct(w_o.shape, jnp.bfloat16)],
        scratch_shapes=[pltpu.VMEM((rows, width), jnp.float32)],
        compiler_params=pltpu.CompilerParams(vmem_limit_bytes=VMEM_LIMIT),
        cost_estimate=pl.CostEstimate(flops=2 * n * rows * cols * width, bytes_accessed=2 * n * cols * (rows + width), transcendentals=0),
        name="out_project",
    )(o_chunks, w_o, dwo_slab)


def add_head(g_ref, wq_ref, wk_ref, wv_ref, acc_ref):
    w_qk = jnp.concatenate([wq_ref[...], wk_ref[...]], axis=1)
    acc_ref[...] += (dot_f32(g_ref[0, :, :2 * HEAD_DIM], w_qk, LAST)
                     + dot_f32(g_ref[0, :, 2 * HEAD_DIM:], wv_ref[...], LAST))


def tail_a_kernel(g_ref, wq_ref, wk_ref, wv_ref, dh_ref):
    @pl.when(pl.program_id(0) == 0)
    def _():
        dh_ref[...] = jnp.zeros_like(dh_ref)

    add_head(g_ref, wq_ref, wk_ref, wv_ref, dh_ref)


def tail_b_kernel(g_ref, wq_ref, wk_ref, wv_ref, first_ref, x_ref, lnw_ref, dx_ref, dlnw_ref, acc_ref):
    d = pl.program_id(0)

    @pl.when(d == 0)
    def _():
        acc_ref[...] = first_ref[...]

    add_head(g_ref, wq_ref, wk_ref, wv_ref, acc_ref)

    @pl.when(d == pl.num_programs(0) - 1)
    def _():
        dlnw_ref[...] = jnp.zeros_like(dlnw_ref)
        lnw = lnw_ref[...]
        step = 64

        def rows_step(t, c):
            rows = pl.ds(pl.multiple_of(t * step, step), step)
            x = x_ref[rows, :].astype(jnp.float32)
            dh = acc_ref[rows, :]
            centered = x - jnp.mean(x, axis=-1, keepdims=True)
            rstd = lax.rsqrt(jnp.mean(centered * centered, axis=-1, keepdims=True) + LN_EPS)
            xhat = centered * rstd
            dlnw_ref[...] += jnp.sum(dh * xhat, axis=0, keepdims=True)
            dxhat = dh * lnw
            dx = rstd * (dxhat - jnp.mean(dxhat, axis=-1, keepdims=True) - xhat * jnp.mean(dxhat * xhat, axis=-1, keepdims=True))
            dx_ref[rows, :] = dx.astype(jnp.bfloat16)
            return c

        lax.fori_loop(0, x_ref.shape[0] // step, rows_step, 0)


def tail(g_chunks, w_q, w_k, w_v, head, heads, rest=()):
    n, rows, cols = g_chunks.shape
    width = w_q.shape[0]
    w_spec = pl.BlockSpec((width, HEAD_DIM), lambda d: (0, heads * d + head))
    whole = pl.BlockSpec((rows, width), lambda d: (0, 0))
    row = pl.BlockSpec((1, width), lambda d: (0, 0))
    dh = jax.ShapeDtypeStruct((rows, width), jnp.float32)
    last = bool(rest)
    return pl.pallas_call(
        tail_b_kernel if last else tail_a_kernel, grid=(n,),
        in_specs=[pl.BlockSpec((1, rows, cols), lambda d: (d, 0, 0)), w_spec, w_spec, w_spec] + ([whole, whole, row] if last else []),
        out_specs=[whole, row] if last else whole,
        out_shape=[jax.ShapeDtypeStruct((rows, width), jnp.bfloat16), jax.ShapeDtypeStruct((1, width), jnp.float32)] if last else dh,
        scratch_shapes=[pltpu.VMEM((rows, width), jnp.float32)] if last else [],
        compiler_params=pltpu.CompilerParams(vmem_limit_bytes=VMEM_LIMIT),
        cost_estimate=pl.CostEstimate(flops=2 * n * rows * cols * width, bytes_accessed=2 * n * cols * (rows + width), transcendentals=0),
        name="tail_b" if last else "tail_a",
    )(g_chunks, w_q, w_k, w_v, *rest)


def assemble_kernel(slab_ref, *refs):
    for part, out in enumerate(refs[-3:]):
        out[...] = slab_ref[0, :, part * HEAD_DIM:(part + 1) * HEAD_DIM]


def assemble(slab, head, heads, into=()):
    n, rows, cols = slab.shape
    out_spec = pl.BlockSpec((rows, HEAD_DIM), lambda d: (0, heads * d + head))
    out = jax.ShapeDtypeStruct((rows, n * heads * HEAD_DIM), jnp.bfloat16)
    return pl.pallas_call(
        assemble_kernel, grid=(n,),
        in_specs=[pl.BlockSpec((1, rows, cols), lambda d: (d, 0, 0))] + [pl.BlockSpec(memory_space=pl.ANY)] * len(into),
        out_specs=[out_spec] * 3, out_shape=[out] * 3,
        input_output_aliases={1 + i: i for i in range(len(into))},
        compiler_params=pltpu.CompilerParams(vmem_limit_bytes=VMEM_LIMIT),
        cost_estimate=pl.CostEstimate(flops=rows * n * cols * 64, bytes_accessed=4 * n * rows * cols, transcendentals=0),
        name="assemble",
    )(slab, *into)


def solution(mesh):
    sp_size = mesh.shape['sp']
    row_spec = P(('dp', 'sp'), None)
    pos_spec = P(('dp', 'sp'))
    full_spec = P(None, None)
    grad_spec = P('dp', None)

    def layer(hidden, positions, d_attn, ln_weight, w_q, w_k, w_v, w_o):
        me = lax.axis_index('sp')
        block = hidden.shape[0]
        cols = w_q.shape[1] // sp_size
        lnw32 = ln_weight.astype(jnp.float32)
        normed = layer_norm(hidden, lnw32[None])
        pos_all = lax.all_gather(positions, 'sp', tiled=True)
        h_all = lax.all_gather(normed, 'sp', tiled=True)
        g_all = lax.all_gather(d_attn, 'sp', tiled=True)
        cos_full, sin_full = rope_tables(pos_all)
        mine = lambda w, axis: lax.dynamic_slice_in_dim(w, me * cols, cols, axis)
        wq_my, wk_my, wv_my, wo_my = mine(w_q, 1), mine(w_k, 1), mine(w_v, 1), mine(w_o, 0)
        q, k, v, kt, vt = project(h_all, wq_my, wk_my, wv_my, cos_full, sin_full)

        def exchange(x):
            return lax.all_to_all(x.reshape(sp_size, block, x.shape[1]), 'sp', 0, 0)

        o, ot, lse = attn_forward(q, k, vt, block)
        o_chunks = exchange(o)
        d_o, dwo_my = cotangents(g_all, wo_my, ot, block)

        def back(q, head):
            return attn_backward(q, d_o, ot, lse, k, v, kt, cos_full, sin_full, block, head)

        def wgrad(x):
            return jnp.einsum('td,te->de', h_all, x, preferred_element_type=jnp.float32).astype(jnp.bfloat16)

        q_0, dwo_my = lax.optimization_barrier((q, dwo_my))
        dwo_slab = lax.all_gather(dwo_my, 'sp', tiled=True)
        g_a = back(q_0, 0)
        sent_a, o_chunks = lax.optimization_barrier((g_a, o_chunks))
        ga_tok = exchange(sent_a)
        q_1, part_a = lax.optimization_barrier((q, wgrad(g_a)))
        slab_a = lax.all_gather(part_a, 'sp')
        g_b = back(q_1, 1)
        sent_b, ga_tok = lax.optimization_barrier((g_b, ga_tok))
        gb_tok = exchange(sent_b)
        part_b = wgrad(g_b)
        slab_b = lax.all_gather(part_b, 'sp')
        ga_tok, o_chunks, dwo_slab, part_b = lax.optimization_barrier((ga_tok, o_chunks, dwo_slab, part_b))
        dh_a = tail(ga_tok, w_q, w_k, w_v, 0, 2)
        attn_out, dw_o = out_project(o_chunks, w_o, dwo_slab)
        dh_a, attn_out, dw_o, slab_a = lax.optimization_barrier((dh_a, attn_out, dw_o, slab_a))
        half = assemble(slab_a, 0, 2)
        d_hid, d_lnw = tail(gb_tok, w_q, w_k, w_v, 1, 2, (dh_a, hidden, lnw32[None]))
        d_lnw = lax.psum(d_lnw[0], 'sp').astype(jnp.bfloat16)
        half, d_hid, d_lnw, attn_out, slab_b = lax.optimization_barrier((half, d_hid, d_lnw, attn_out, slab_b))
        dw_q, dw_k, dw_v = assemble(slab_b, 1, 2, half)
        return attn_out, d_hid, d_lnw, dw_q, dw_k, dw_v, dw_o

    return jax.shard_map(layer, mesh=mesh,
                         in_specs=(row_spec, pos_spec, row_spec, P(None), full_spec, full_spec, full_spec, full_spec),
                         out_specs=(row_spec, row_spec, P('dp'), grad_spec, grad_spec, grad_spec, grad_spec),
                         check_vma=False)
```

```python
import math
import jax
import jax.numpy as jnp
from jax import lax
from jax.experimental import pallas as pl
from jax.experimental.pallas import tpu as pltpu
from jax.sharding import PartitionSpec as P

HEAD_DIM = 128
LN_EPS = 1e-5
ROPE_BASE = 10000.0
SCALE = HEAD_DIM ** -0.5
EXP2_SCALE = SCALE * math.log2(math.e)
SUB = 256
CORES = 2
VMEM_LIMIT = 56 * 1024 * 1024
LAST = (((1,), (1,)), ((), ()))
PLAIN = (((1,), (0,)), ((), ()))


def norm_f32(hid_f32, weight_f32):
    mean_val = jnp.mean(hid_f32, axis=-1, keepdims=True)
    centered = hid_f32 - mean_val
    var_val = jnp.mean(centered * centered, axis=-1, keepdims=True)
    return centered * lax.rsqrt(var_val + LN_EPS) * weight_f32


def ln_kernel(x_ref, w_ref, h_ref):
    h_ref[...] = norm_f32(x_ref[...].astype(jnp.float32), w_ref[...]).astype(jnp.bfloat16)


def layer_norm(x, ln_weight):
    rows, width = x.shape
    tile = math.gcd(rows, 128)
    spec = pl.BlockSpec((tile, width), lambda i: (i, 0))
    return pl.pallas_call(
        ln_kernel, grid=(rows // tile,),
        in_specs=[spec, pl.BlockSpec((1, width), lambda i: (0, 0))], out_specs=spec,
        out_shape=jax.ShapeDtypeStruct(x.shape, jnp.bfloat16),
        compiler_params=pltpu.CompilerParams(vmem_limit_bytes=VMEM_LIMIT),
        cost_estimate=pl.CostEstimate(flops=10 * rows * width, bytes_accessed=4 * rows * width, transcendentals=0),
        name="layer_norm",
    )(x, ln_weight)


def rope_tables(positions):
    lane = jnp.arange(HEAD_DIM)
    inv_freq = ROPE_BASE ** (-(lane - lane % 2).astype(jnp.float32) / HEAD_DIM)
    angles = positions.astype(jnp.float32)[:, None] * inv_freq[None, :]
    sin_t = jnp.sin(angles)
    return jnp.cos(angles), jnp.where(lane % 2 == 0, -sin_t, sin_t)


def swap_pairs(x):
    lane = lax.broadcasted_iota(jnp.int32, x.shape, 1)
    up = pltpu.roll(x, HEAD_DIM - 1, 1)
    down = pltpu.roll(x, 1, 1)
    return jnp.where(lane % 2 == 0, up, down)


def dot_f32(a, b, dims):
    return lax.dot_general(a, b, dims, preferred_element_type=jnp.float32)


def proj_kernel(core_ref, h_ref, wq_ref, wk_ref, wv_ref, cos_ref, sin_ref, *refs):
    q_ref, k_ref, v_ref, kt_ref, vt_ref = refs[-5:]
    h = h_ref[0]
    cos_t, sin_t = cos_ref[...], sin_ref[...]
    q = dot_f32(h, wq_ref[...], PLAIN)
    k = dot_f32(h, wk_ref[...], PLAIN)
    v = dot_f32(h, wv_ref[...], PLAIN)
    for n in range(q.shape[1] // HEAD_DIM):
        cols = slice(n * HEAD_DIM, (n + 1) * HEAD_DIM)
        qn, kn, vn = q[:, cols], k[:, cols], v[:, cols]
        q_ref[:, cols] = (qn * cos_t + swap_pairs(qn) * sin_t).astype(jnp.bfloat16)
        kn = kn * cos_t + swap_pairs(kn) * sin_t
        k_ref[:, cols] = kn.astype(jnp.bfloat16)
        v_ref[:, cols] = vn.astype(jnp.bfloat16)
        kt_ref[cols, :] = kn.T.astype(jnp.bfloat16)
        vt_ref[cols, :] = vn.T.astype(jnp.bfloat16)


def project(h_half, core, w_q, w_k, w_v, cos_full, sin_full, into=()):
    chips, block, depth = h_half.shape
    rows = chips * CORES * block
    cols = w_q.shape[1]
    row_spec = lambda width: pl.BlockSpec((block, width), lambda c, core: (CORES * c + core[0], 0))
    full = pl.BlockSpec((depth, cols), lambda c, core: (0, 0))
    col_spec = pl.BlockSpec((cols, block), lambda c, core: (0, CORES * c + core[0]))
    out = jax.ShapeDtypeStruct((rows, cols), jnp.bfloat16)
    out_t = jax.ShapeDtypeStruct((cols, rows), jnp.bfloat16)
    return pl.pallas_call(
        proj_kernel,
        grid_spec=pltpu.PrefetchScalarGridSpec(
            num_scalar_prefetch=1, grid=(chips,),
            in_specs=[pl.BlockSpec((1, block, depth), lambda c, core: (c, 0, 0)), full, full, full,
                      row_spec(HEAD_DIM), row_spec(HEAD_DIM)] + [pl.BlockSpec(memory_space=pl.ANY)] * len(into),
            out_specs=[row_spec(cols)] * 3 + [col_spec] * 2),
        out_shape=[out] * 3 + [out_t] * 2,
        input_output_aliases={7 + i: i for i in range(len(into))},
        compiler_params=pltpu.CompilerParams(vmem_limit_bytes=VMEM_LIMIT),
        cost_estimate=pl.CostEstimate(flops=6 * chips * block * depth * cols, bytes_accessed=2 * chips * block * (depth + 5 * cols), transcendentals=0),
        name="project",
    )(core, h_half, w_q, w_k, w_v, cos_full, sin_full, *into)


def causal(st, row0, col0):
    keys = lax.broadcasted_iota(jnp.int32, st.shape, 0) + row0
    qs = lax.broadcasted_iota(jnp.int32, st.shape, 1) + col0
    return jnp.where(keys <= qs, st, -jnp.inf)


def fwd_kernel(q_ref, k_ref, vt_ref, o_ref, ot_ref, lse_ref, acc_ref, m_ref, l_ref):
    i = pl.program_id(1)
    rows = q_ref.shape[0]
    acc_ref[...] = jnp.zeros_like(acc_ref)
    m_ref[...] = jnp.full_like(m_ref, -jnp.inf)
    l_ref[...] = jnp.zeros_like(l_ref)

    def step(j, diagonal):
        start = pl.multiple_of(j * rows, rows)

        def scores(a):
            keys = a + SUB if diagonal else rows
            st = dot_f32(k_ref[pl.ds(start, keys), :], q_ref[a:a + SUB, :], LAST)
            return causal(st, 0, a) if diagonal else st

        def update(a, st):
            cols = slice(a, a + SUB)
            m = m_ref[:, cols]
            m_new = jnp.maximum(m, jnp.max(st, axis=0, keepdims=True))
            p = jnp.exp2((st - m_new) * EXP2_SCALE)
            alpha = jnp.exp2((m - m_new) * EXP2_SCALE)
            m_ref[:, cols] = m_new
            l_ref[:, cols] = l_ref[:, cols] * alpha + jnp.sum(p, axis=0, keepdims=True)
            pv = dot_f32(vt_ref[:, pl.ds(start, st.shape[0])], p.astype(jnp.bfloat16), PLAIN)
            acc_ref[:, cols] = acc_ref[:, cols] * alpha + pv

        st = scores(0)
        for a in range(0, rows, SUB):
            ahead = scores(a + SUB) if a + SUB < rows else None
            update(a, st)
            st = ahead

    lax.fori_loop(0, i, lambda j, c: (step(j, False), c)[1], 0)
    step(i, True)
    ot = acc_ref[...] / l_ref[...]
    ot_ref[...] = ot
    o_ref[...] = ot.T.astype(jnp.bfloat16)
    lse_ref[0] = m_ref[...] * EXP2_SCALE + jnp.log2(l_ref[...])


def attn_forward(q, k, vt, block):
    rows, cols = q.shape
    heads = cols // HEAD_DIM
    flops = 2 * 2 * rows * rows * cols // 2
    return pl.pallas_call(
        fwd_kernel, grid=(heads, rows // block),
        in_specs=[pl.BlockSpec((block, HEAD_DIM), lambda h, i: (i, h)),
                  pl.BlockSpec((rows, HEAD_DIM), lambda h, i: (0, h)),
                  pl.BlockSpec((HEAD_DIM, rows), lambda h, i: (h, 0))],
        out_specs=[pl.BlockSpec((block, HEAD_DIM), lambda h, i: (i, h)),
                   pl.BlockSpec((HEAD_DIM, block), lambda h, i: (h, i)),
                   pl.BlockSpec((1, 1, block), lambda h, i: (h, 0, i))],
        out_shape=[jax.ShapeDtypeStruct((rows, cols), jnp.bfloat16),
                   jax.ShapeDtypeStruct((cols, rows), jnp.float32),
                   jax.ShapeDtypeStruct((heads, 1, rows), jnp.float32)],
        scratch_shapes=[pltpu.VMEM((HEAD_DIM, block), jnp.float32),
                        pltpu.VMEM((1, block), jnp.float32),
                        pltpu.VMEM((1, block), jnp.float32)],
        compiler_params=pltpu.CompilerParams(vmem_limit_bytes=VMEM_LIMIT),
        cost_estimate=pl.CostEstimate(flops=2 * flops, bytes_accessed=10 * rows * cols, transcendentals=0),
        name="attn_fwd",
    )(q, k, vt)


def unrope(x, cos_t, sin_t):
    x = x.astype(jnp.bfloat16).astype(jnp.float32)
    return (x * cos_t - swap_pairs(x) * sin_t).astype(jnp.bfloat16)


def bwd_kernel(q_ref, do_ref, ot_ref, lse_ref, k_ref, v_ref, kt_ref, cos_ref, sin_ref,
               g_ref, dk_acc, dv_acc, dqt_acc):
    i = pl.program_id(0)
    rows = q_ref.shape[0]

    @pl.when(i == 0)
    def _():
        dk_acc[...] = jnp.zeros_like(dk_acc)
        dv_acc[...] = jnp.zeros_like(dv_acc)

    lse = lse_ref[0]
    row_dot = jnp.sum(do_ref[...].astype(jnp.float32).T * ot_ref[...], axis=0, keepdims=True)
    dqt_acc[...] = jnp.zeros_like(dqt_acc)

    def step(j, diagonal):
        start = pl.multiple_of(j * rows, rows)

        def scores(b):
            first = b if diagonal else 0
            keys = pl.ds(start + b, SUB)
            st = dot_f32(k_ref[keys, :], q_ref[first:, :], LAST)
            dpt = dot_f32(v_ref[keys, :], do_ref[first:, :], LAST)
            return st, dpt

        def update(b, st, dpt):
            first = b if diagonal else 0
            keys = pl.ds(start + b, SUB)
            if diagonal:
                st = causal(st, b, first)
            p = jnp.exp2(st * EXP2_SCALE - lse[:, first:])
            ds = (p * (dpt - row_dot[:, first:]) * SCALE).astype(jnp.bfloat16)
            dv_acc[keys, :] += dot_f32(p.astype(jnp.bfloat16), do_ref[first:, :], PLAIN)
            dk_acc[keys, :] += dot_f32(ds, q_ref[first:, :], PLAIN)
            dqt_acc[:, first:] += dot_f32(kt_ref[:, keys], ds, PLAIN)

        now = scores(0)
        for b in range(0, rows, SUB):
            ahead = scores(b + SUB) if b + SUB < rows else None
            update(b, *now)
            now = ahead

    lax.fori_loop(0, i, lambda j, c: (step(j, False), c)[1], 0)
    step(i, True)
    tile = pl.ds(pl.multiple_of(i * rows, rows), rows)
    g_ref[tile, :HEAD_DIM] = unrope(dqt_acc[...].T, cos_ref[tile, :], sin_ref[tile, :])

    @pl.when(i == pl.num_programs(0) - 1)
    def _():
        def finish(j, c):
            part = pl.ds(pl.multiple_of(j * rows, rows), rows)
            g_ref[part, HEAD_DIM:2 * HEAD_DIM] = unrope(dk_acc[part, :], cos_ref[part, :], sin_ref[part, :])
            g_ref[part, 2 * HEAD_DIM:] = dv_acc[part, :].astype(jnp.bfloat16)
            return c

        lax.fori_loop(0, dk_acc.shape[0] // rows, finish, 0)


def attn_backward(q, do, ot, lse, k, v, kt, cos_full, sin_full, block, head):
    rows = q.shape[0]
    flops = 2 * rows * rows * HEAD_DIM // 2
    q_spec = pl.BlockSpec((block, HEAD_DIM), lambda i: (i, head))
    all_spec = pl.BlockSpec((rows, HEAD_DIM), lambda i: (0, head))
    table = pl.BlockSpec((rows, HEAD_DIM), lambda i: (0, 0))
    return pl.pallas_call(
        bwd_kernel, grid=(rows // block,),
        in_specs=[q_spec, q_spec,
                  pl.BlockSpec((HEAD_DIM, block), lambda i: (head, i)),
                  pl.BlockSpec((1, 1, block), lambda i: (head, 0, i)),
                  all_spec, all_spec,
                  pl.BlockSpec((HEAD_DIM, rows), lambda i: (head, 0)),
                  table, table],
        out_specs=pl.BlockSpec((rows, 3 * HEAD_DIM), lambda i: (0, 0)),
        out_shape=jax.ShapeDtypeStruct((rows, 3 * HEAD_DIM), jnp.bfloat16),
        scratch_shapes=[pltpu.VMEM((rows, HEAD_DIM), jnp.float32),
                        pltpu.VMEM((rows, HEAD_DIM), jnp.float32),
                        pltpu.VMEM((HEAD_DIM, block), jnp.float32)],
        compiler_params=pltpu.CompilerParams(vmem_limit_bytes=VMEM_LIMIT),
        cost_estimate=pl.CostEstimate(flops=2 * 5 * flops, bytes_accessed=20 * rows * HEAD_DIM, transcendentals=0),
        name="attn_bwd",
    )(q, do, ot, lse, k, v, kt, cos_full, sin_full)


def cot_kernel(g_ref, w_ref, ot_ref, do_ref, dw_ref, acc_ref):
    t = pl.program_id(0)

    @pl.when(t == 0)
    def _():
        acc_ref[...] = jnp.zeros_like(acc_ref)

    g = g_ref[...]
    do_ref[...] = dot_f32(g, w_ref[...], LAST).astype(jnp.bfloat16)
    acc_ref[...] += dot_f32(ot_ref[...].astype(jnp.bfloat16), g, PLAIN)

    @pl.when(t == pl.num_programs(0) - 1)
    def _():
        dw_ref[...] = acc_ref[...].astype(jnp.bfloat16)


def cotangents(g_all, wo_my, ot, block):
    rows, width = g_all.shape
    cols = wo_my.shape[0]
    slab = pl.BlockSpec((cols, width), lambda t: (0, 0))
    return pl.pallas_call(
        cot_kernel, grid=(rows // block,),
        in_specs=[pl.BlockSpec((block, width), lambda t: (t, 0)), slab, pl.BlockSpec((cols, block), lambda t: (0, t))],
        out_specs=[pl.BlockSpec((block, cols), lambda t: (t, 0)), slab],
        out_shape=[jax.ShapeDtypeStruct((rows, cols), jnp.bfloat16), jax.ShapeDtypeStruct((cols, width), jnp.bfloat16)],
        scratch_shapes=[pltpu.VMEM((cols, width), jnp.float32)],
        compiler_params=pltpu.CompilerParams(vmem_limit_bytes=VMEM_LIMIT),
        cost_estimate=pl.CostEstimate(flops=4 * rows * cols * width, bytes_accessed=2 * rows * (width + 3 * cols), transcendentals=0),
        name="cotangents",
    )(g_all, wo_my, ot)


def out_kernel(o_ref, w_ref, slab_ref, a_ref, dwo_ref, acc_ref):
    d = pl.program_id(0)
    dwo_ref[...] = slab_ref[...]

    @pl.when(d == 0)
    def _():
        acc_ref[...] = jnp.zeros_like(acc_ref)

    acc_ref[...] += dot_f32(o_ref[0], w_ref[...], PLAIN)

    @pl.when(d == pl.num_programs(0) - 1)
    def _():
        a_ref[...] = acc_ref[...].astype(jnp.bfloat16)


def out_project(o_chunks, w_o, dwo_slab):
    n, rows, cols = o_chunks.shape
    width = w_o.shape[1]
    return pl.pallas_call(
        out_kernel, grid=(n,),
        in_specs=[pl.BlockSpec((1, rows, cols), lambda d: (d, 0, 0)),
                  pl.BlockSpec((cols, width), lambda d: (d, 0)),
                  pl.BlockSpec((cols, width), lambda d: (d, 0))],
        out_specs=[pl.BlockSpec((rows, width), lambda d: (0, 0)),
                   pl.BlockSpec((cols, width), lambda d: (d, 0))],
        out_shape=[jax.ShapeDtypeStruct((rows, width), jnp.bfloat16),
                   jax.ShapeDtypeStruct(w_o.shape, jnp.bfloat16)],
        scratch_shapes=[pltpu.VMEM((rows, width), jnp.float32)],
        compiler_params=pltpu.CompilerParams(vmem_limit_bytes=VMEM_LIMIT),
        cost_estimate=pl.CostEstimate(flops=2 * n * rows * cols * width, bytes_accessed=2 * n * cols * (rows + width), transcendentals=0),
        name="out_project",
    )(o_chunks, w_o, dwo_slab)


def add_head(g_ref, wq_ref, wk_ref, wv_ref, acc_ref):
    w_qk = jnp.concatenate([wq_ref[...], wk_ref[...]], axis=1)
    acc_ref[...] += (dot_f32(g_ref[0, :, :2 * HEAD_DIM], w_qk, LAST)
                     + dot_f32(g_ref[0, :, 2 * HEAD_DIM:], wv_ref[...], LAST))


def tail_a_kernel(g_ref, wq_ref, wk_ref, wv_ref, dh_ref):
    @pl.when(pl.program_id(0) == 0)
    def _():
        dh_ref[...] = jnp.zeros_like(dh_ref)

    add_head(g_ref, wq_ref, wk_ref, wv_ref, dh_ref)


def tail_b_kernel(g_ref, wq_ref, wk_ref, wv_ref, first_ref, x_ref, lnw_ref, dx_ref, dlnw_ref, acc_ref):
    d = pl.program_id(0)

    @pl.when(d == 0)
    def _():
        acc_ref[...] = first_ref[...]

    add_head(g_ref, wq_ref, wk_ref, wv_ref, acc_ref)

    @pl.when(d == pl.num_programs(0) - 1)
    def _():
        dlnw_ref[...] = jnp.zeros_like(dlnw_ref)
        lnw = lnw_ref[...]
        step = 64

        def rows_step(t, c):
            rows = pl.ds(pl.multiple_of(t * step, step), step)
            x = x_ref[rows, :].astype(jnp.float32)
            dh = acc_ref[rows, :]
            centered = x - jnp.mean(x, axis=-1, keepdims=True)
            rstd = lax.rsqrt(jnp.mean(centered * centered, axis=-1, keepdims=True) + LN_EPS)
            xhat = centered * rstd
            dlnw_ref[...] += jnp.sum(dh * xhat, axis=0, keepdims=True)
            dxhat = dh * lnw
            dx = rstd * (dxhat - jnp.mean(dxhat, axis=-1, keepdims=True) - xhat * jnp.mean(dxhat * xhat, axis=-1, keepdims=True))
            dx_ref[rows, :] = dx.astype(jnp.bfloat16)
            return c

        lax.fori_loop(0, x_ref.shape[0] // step, rows_step, 0)


def tail(g_chunks, w_q, w_k, w_v, head, heads, rest=()):
    n, rows, cols = g_chunks.shape
    width = w_q.shape[0]
    w_spec = pl.BlockSpec((width, HEAD_DIM), lambda d: (0, heads * d + head))
    whole = pl.BlockSpec((rows, width), lambda d: (0, 0))
    row = pl.BlockSpec((1, width), lambda d: (0, 0))
    dh = jax.ShapeDtypeStruct((rows, width), jnp.float32)
    last = bool(rest)
    return pl.pallas_call(
        tail_b_kernel if last else tail_a_kernel, grid=(n,),
        in_specs=[pl.BlockSpec((1, rows, cols), lambda d: (d, 0, 0)), w_spec, w_spec, w_spec] + ([whole, whole, row] if last else []),
        out_specs=[whole, row] if last else whole,
        out_shape=[jax.ShapeDtypeStruct((rows, width), jnp.bfloat16), jax.ShapeDtypeStruct((1, width), jnp.float32)] if last else dh,
        scratch_shapes=[pltpu.VMEM((rows, width), jnp.float32)] if last else [],
        compiler_params=pltpu.CompilerParams(vmem_limit_bytes=VMEM_LIMIT),
        cost_estimate=pl.CostEstimate(flops=2 * n * rows * cols * width, bytes_accessed=2 * n * cols * (rows + width), transcendentals=0),
        name="tail_b" if last else "tail_a",
    )(g_chunks, w_q, w_k, w_v, *rest)


def assemble_kernel(slab_ref, *refs):
    for part, out in enumerate(refs[-3:]):
        out[...] = slab_ref[0, :, part * HEAD_DIM:(part + 1) * HEAD_DIM]


def assemble(slab, head, heads, into=()):
    n, rows, cols = slab.shape
    out_spec = pl.BlockSpec((rows, HEAD_DIM), lambda d: (0, heads * d + head))
    out = jax.ShapeDtypeStruct((rows, n * heads * HEAD_DIM), jnp.bfloat16)
    return pl.pallas_call(
        assemble_kernel, grid=(n,),
        in_specs=[pl.BlockSpec((1, rows, cols), lambda d: (d, 0, 0))] + [pl.BlockSpec(memory_space=pl.ANY)] * len(into),
        out_specs=[out_spec] * 3, out_shape=[out] * 3,
        input_output_aliases={1 + i: i for i in range(len(into))},
        compiler_params=pltpu.CompilerParams(vmem_limit_bytes=VMEM_LIMIT),
        cost_estimate=pl.CostEstimate(flops=rows * n * cols * 64, bytes_accessed=4 * n * rows * cols, transcendentals=0),
        name="assemble",
    )(slab, *into)


def solution(mesh):
    sp_size = mesh.shape['sp']
    row_spec = P(('dp', 'sp'), None)
    pos_spec = P(('dp', 'sp'))
    full_spec = P(None, None)
    grad_spec = P('dp', None)

    def layer(hidden, positions, d_attn, ln_weight, w_q, w_k, w_v, w_o):
        me = lax.axis_index('sp')
        block = hidden.shape[0]
        cols = w_q.shape[1] // sp_size
        lnw32 = ln_weight.astype(jnp.float32)
        normed = layer_norm(hidden, lnw32[None])
        pos_all = lax.all_gather(positions, 'sp', tiled=True)
        same_core = [[d for d in range(sp_size) if d % CORES == c] for c in range(CORES)]
        normed, d_attn = lax.optimization_barrier((normed, d_attn))
        h_own = lax.all_gather(normed, 'sp', axis_index_groups=same_core)
        cos_full, sin_full = rope_tables(pos_all)
        mine = lambda w, axis: lax.dynamic_slice_in_dim(w, me * cols, cols, axis)
        wq_my, wk_my, wv_my, wo_my = mine(w_q, 1), mine(w_k, 1), mine(w_v, 1), mine(w_o, 0)
        h_own, cos_full, sin_full, wq_my, wk_my, wv_my, wo_my = lax.optimization_barrier(
            (h_own, cos_full, sin_full, wq_my, wk_my, wv_my, wo_my))
        h_other = lax.ppermute(h_own, 'sp', [(d, d ^ 1) for d in range(sp_size)])
        g_all = lax.all_gather(d_attn, 'sp', tiled=True)
        core = (me % CORES).astype(jnp.int32)
        partner = CORES - 1 - core
        mine_done = project(h_own, core[None], wq_my, wk_my, wv_my, cos_full, sin_full)
        q, k, v, kt, vt = project(h_other, partner[None], wq_my, wk_my, wv_my, cos_full, sin_full, mine_done)

        def exchange(x):
            return lax.all_to_all(x.reshape(sp_size, block, x.shape[1]), 'sp', 0, 0)

        o, ot, lse = attn_forward(q, k, vt, block)
        o_chunks = exchange(o)
        d_o, dwo_my = cotangents(g_all, wo_my, ot, block)

        def back(q, head):
            return attn_backward(q, d_o, ot, lse, k, v, kt, cos_full, sin_full, block, head)

        def wgrad(x):
            blocks = x.reshape(sp_size // CORES, CORES, block, x.shape[1])
            half = lambda h, c: jnp.einsum('ctd,cte->de', h, lax.dynamic_index_in_dim(blocks, c, 1, False), preferred_element_type=jnp.float32)
            return (half(h_own, core) + half(h_other, partner)).astype(jnp.bfloat16)

        q_0, dwo_my = lax.optimization_barrier((q, dwo_my))
        dwo_slab = lax.all_gather(dwo_my, 'sp', tiled=True)
        g_a = back(q_0, 0)
        sent_a, o_chunks = lax.optimization_barrier((g_a, o_chunks))
        ga_tok = exchange(sent_a)
        q_1, part_a = lax.optimization_barrier((q, wgrad(g_a)))
        slab_a = lax.all_gather(part_a, 'sp')
        g_b = back(q_1, 1)
        sent_b, ga_tok = lax.optimization_barrier((g_b, ga_tok))
        gb_tok = exchange(sent_b)
        part_b = wgrad(g_b)
        slab_b = lax.all_gather(part_b, 'sp')
        ga_tok, o_chunks, dwo_slab, part_b = lax.optimization_barrier((ga_tok, o_chunks, dwo_slab, part_b))
        dh_a = tail(ga_tok, w_q, w_k, w_v, 0, 2)
        attn_out, dw_o = out_project(o_chunks, w_o, dwo_slab)
        dh_a, attn_out, dw_o, slab_a = lax.optimization_barrier((dh_a, attn_out, dw_o, slab_a))
        half = assemble(slab_a, 0, 2)
        d_hid, d_lnw = tail(gb_tok, w_q, w_k, w_v, 1, 2, (dh_a, hidden, lnw32[None]))
        parts = lax.all_to_all(jnp.broadcast_to(d_lnw[None], (sp_size,) + d_lnw.shape), 'sp', 0, 0)
        d_lnw = jnp.sum(parts, axis=(0, 1)).astype(jnp.bfloat16)
        half, d_hid, attn_out, slab_b = lax.optimization_barrier((half, d_hid, attn_out, slab_b))
        dw_q, dw_k, dw_v = assemble(slab_b, 1, 2, half)
        return attn_out, d_hid, d_lnw, dw_q, dw_k, dw_v, dw_o

    return jax.shard_map(layer, mesh=mesh,
                         in_specs=(row_spec, pos_spec, row_spec, P(None), full_spec, full_spec, full_spec, full_spec),
                         out_specs=(row_spec, row_spec, P('dp'), grad_spec, grad_spec, grad_spec, grad_spec),
                         check_vma=False)
```

```python
import math
import jax
import jax.numpy as jnp
from jax import lax
from jax.experimental import pallas as pl
from jax.experimental.pallas import tpu as pltpu
from jax.sharding import PartitionSpec as P

HEAD_DIM = 128
LN_EPS = 1e-5
ROPE_BASE = 10000.0
SCALE = HEAD_DIM ** -0.5
EXP2_SCALE = SCALE * math.log2(math.e)
BLOCK = 512
SUB = 256
VMEM_LIMIT = 56 * 1024 * 1024
LAST = (((1,), (1,)), ((), ()))
PLAIN = (((1,), (0,)), ((), ()))


def norm_f32(hid_f32, weight_f32):
    mean_val = jnp.mean(hid_f32, axis=-1, keepdims=True)
    centered = hid_f32 - mean_val
    var_val = jnp.mean(centered * centered, axis=-1, keepdims=True)
    return centered * lax.rsqrt(var_val + LN_EPS) * weight_f32


def ln_kernel(x_ref, w_ref, h_ref):
    h_ref[...] = norm_f32(x_ref[...].astype(jnp.float32), w_ref[...]).astype(jnp.bfloat16)


def layer_norm(x, ln_weight):
    rows, width = x.shape
    tile = math.gcd(rows, 128)
    spec = pl.BlockSpec((tile, width), lambda i: (i, 0))
    return pl.pallas_call(
        ln_kernel, grid=(rows // tile,),
        in_specs=[spec, pl.BlockSpec((1, width), lambda i: (0, 0))], out_specs=spec,
        out_shape=jax.ShapeDtypeStruct(x.shape, jnp.bfloat16),
        compiler_params=pltpu.CompilerParams(vmem_limit_bytes=VMEM_LIMIT),
        cost_estimate=pl.CostEstimate(flops=10 * rows * width, bytes_accessed=4 * rows * width, transcendentals=0),
        name="layer_norm",
    )(x, ln_weight)


def rope_tables(positions):
    lane = jnp.arange(HEAD_DIM)
    inv_freq = ROPE_BASE ** (-(lane - lane % 2).astype(jnp.float32) / HEAD_DIM)
    angles = positions.astype(jnp.float32)[:, None] * inv_freq[None, :]
    sin_t = jnp.sin(angles)
    return jnp.cos(angles), jnp.where(lane % 2 == 0, -sin_t, sin_t)


def swap_pairs(x):
    lane = lax.broadcasted_iota(jnp.int32, x.shape, 1)
    up = pltpu.roll(x, HEAD_DIM - 1, 1)
    down = pltpu.roll(x, 1, 1)
    return jnp.where(lane % 2 == 0, up, down)


def dot_f32(a, b, dims):
    return lax.dot_general(a, b, dims, preferred_element_type=jnp.float32)


def proj_kernel(h_ref, wq_ref, wk_ref, wv_ref, cos_ref, sin_ref, q_ref, k_ref, v_ref, kt_ref, vt_ref):
    h = h_ref[...]
    cos_t, sin_t = cos_ref[...], sin_ref[...]
    q = dot_f32(h, wq_ref[...], PLAIN)
    k = dot_f32(h, wk_ref[...], PLAIN)
    v = dot_f32(h, wv_ref[...], PLAIN)
    for n in range(q.shape[1] // HEAD_DIM):
        cols = slice(n * HEAD_DIM, (n + 1) * HEAD_DIM)
        qn, kn, vn = q[:, cols], k[:, cols], v[:, cols]
        q_ref[:, cols] = (qn * cos_t + swap_pairs(qn) * sin_t).astype(jnp.bfloat16)
        kn = kn * cos_t + swap_pairs(kn) * sin_t
        k_ref[:, cols] = kn.astype(jnp.bfloat16)
        v_ref[:, cols] = vn.astype(jnp.bfloat16)
        kt_ref[cols, :] = kn.T.astype(jnp.bfloat16)
        vt_ref[cols, :] = vn.T.astype(jnp.bfloat16)


def project(h_all, w_q, w_k, w_v, cos_full, sin_full):
    rows, depth = h_all.shape
    cols = w_q.shape[1]
    tile = BLOCK
    row_spec = lambda width: pl.BlockSpec((tile, width), lambda i: (i, 0))
    full = pl.BlockSpec((depth, cols), lambda i: (0, 0))
    col_spec = pl.BlockSpec((cols, tile), lambda i: (0, i))
    out = jax.ShapeDtypeStruct((rows, cols), jnp.bfloat16)
    out_t = jax.ShapeDtypeStruct((cols, rows), jnp.bfloat16)
    return pl.pallas_call(
        proj_kernel, grid=(rows // tile,),
        in_specs=[row_spec(depth), full, full, full, row_spec(HEAD_DIM), row_spec(HEAD_DIM)],
        out_specs=[row_spec(cols)] * 3 + [col_spec] * 2,
        out_shape=[out] * 3 + [out_t] * 2,
        compiler_params=pltpu.CompilerParams(vmem_limit_bytes=VMEM_LIMIT),
        cost_estimate=pl.CostEstimate(flops=6 * rows * depth * cols, bytes_accessed=2 * rows * (depth + 5 * cols), transcendentals=0),
        name="project",
    )(h_all, w_q, w_k, w_v, cos_full, sin_full)


def causal(st, row0, col0):
    keys = lax.broadcasted_iota(jnp.int32, st.shape, 0) + row0
    qs = lax.broadcasted_iota(jnp.int32, st.shape, 1) + col0
    return jnp.where(keys <= qs, st, -jnp.inf)


def fwd_kernel(q_ref, k_ref, vt_ref, o_ref, ot_ref, lse_ref, acc_ref, m_ref, l_ref):
    i = pl.program_id(1)
    rows = q_ref.shape[0]
    acc_ref[...] = jnp.zeros_like(acc_ref)
    m_ref[...] = jnp.full_like(m_ref, -jnp.inf)
    l_ref[...] = jnp.zeros_like(l_ref)

    def step(j, diagonal):
        start = pl.multiple_of(j * rows, rows)

        def scores(a):
            keys = a + SUB if diagonal else rows
            st = dot_f32(k_ref[pl.ds(start, keys), :], q_ref[a:a + SUB, :], LAST)
            return causal(st, 0, a) if diagonal else st

        def update(a, st):
            cols = slice(a, a + SUB)
            m = m_ref[:, cols]
            m_new = jnp.maximum(m, jnp.max(st, axis=0, keepdims=True))
            p = jnp.exp2((st - m_new) * EXP2_SCALE)
            alpha = jnp.exp2((m - m_new) * EXP2_SCALE)
            m_ref[:, cols] = m_new
            l_ref[:, cols] = l_ref[:, cols] * alpha + jnp.sum(p, axis=0, keepdims=True)
            pv = dot_f32(vt_ref[:, pl.ds(start, st.shape[0])], p.astype(jnp.bfloat16), PLAIN)
            acc_ref[:, cols] = acc_ref[:, cols] * alpha + pv

        st = scores(0)
        for a in range(0, rows, SUB):
            ahead = scores(a + SUB) if a + SUB < rows else None
            update(a, st)
            st = ahead

    lax.fori_loop(0, i, lambda j, c: (step(j, False), c)[1], 0)
    step(i, True)
    ot = acc_ref[...] / l_ref[...]
    ot_ref[...] = ot
    o_ref[...] = ot.T.astype(jnp.bfloat16)
    lse_ref[0] = m_ref[...] * EXP2_SCALE + jnp.log2(l_ref[...])


def attn_forward(q, k, vt, block):
    rows, cols = q.shape
    heads = cols // HEAD_DIM
    flops = 2 * 2 * rows * rows * cols // 2
    return pl.pallas_call(
        fwd_kernel, grid=(heads, rows // block),
        in_specs=[pl.BlockSpec((block, HEAD_DIM), lambda h, i: (i, h)),
                  pl.BlockSpec((rows, HEAD_DIM), lambda h, i: (0, h)),
                  pl.BlockSpec((HEAD_DIM, rows), lambda h, i: (h, 0))],
        out_specs=[pl.BlockSpec((block, HEAD_DIM), lambda h, i: (i, h)),
                   pl.BlockSpec((HEAD_DIM, block), lambda h, i: (h, i)),
                   pl.BlockSpec((1, 1, block), lambda h, i: (h, 0, i))],
        out_shape=[jax.ShapeDtypeStruct((rows, cols), jnp.bfloat16),
                   jax.ShapeDtypeStruct((cols, rows), jnp.float32),
                   jax.ShapeDtypeStruct((heads, 1, rows), jnp.float32)],
        scratch_shapes=[pltpu.VMEM((HEAD_DIM, block), jnp.float32),
                        pltpu.VMEM((1, block), jnp.float32),
                        pltpu.VMEM((1, block), jnp.float32)],
        compiler_params=pltpu.CompilerParams(vmem_limit_bytes=VMEM_LIMIT),
        cost_estimate=pl.CostEstimate(flops=2 * flops, bytes_accessed=10 * rows * cols, transcendentals=0),
        name="attn_fwd",
    )(q, k, vt)


def unrope(x, cos_t, sin_t):
    x = x.astype(jnp.bfloat16).astype(jnp.float32)
    return (x * cos_t - swap_pairs(x) * sin_t).astype(jnp.bfloat16)


def bwd_kernel(q_ref, do_ref, ot_ref, lse_ref, k_ref, v_ref, kt_ref, cos_ref, sin_ref,
               g_ref, dk_acc, dv_acc, dqt_acc, cos_buf, sin_buf, sems):
    i = pl.program_id(0)
    rows = q_ref.shape[0]
    fetches = [pltpu.make_async_copy(cos_ref, cos_buf, sems.at[0]), pltpu.make_async_copy(sin_ref, sin_buf, sems.at[1])]

    @pl.when(i == 0)
    def _():
        for fetch in fetches:
            fetch.start()
        dk_acc[...] = jnp.zeros_like(dk_acc)
        dv_acc[...] = jnp.zeros_like(dv_acc)

    lse = lse_ref[0]
    row_dot = jnp.sum(do_ref[...].astype(jnp.float32).T * ot_ref[...], axis=0, keepdims=True)
    dqt_acc[...] = jnp.zeros_like(dqt_acc)

    def step(j, diagonal):
        start = pl.multiple_of(j * rows, rows)

        def scores(b):
            first = b if diagonal else 0
            keys = pl.ds(start + b, SUB)
            st = dot_f32(k_ref[keys, :], q_ref[first:, :], LAST)
            dpt = dot_f32(v_ref[keys, :], do_ref[first:, :], LAST)
            return st, dpt

        def update(b, st, dpt):
            first = b if diagonal else 0
            keys = pl.ds(start + b, SUB)
            if diagonal:
                st = causal(st, b, first)
            p = jnp.exp2(st * EXP2_SCALE - lse[:, first:])
            ds = (p * (dpt - row_dot[:, first:]) * SCALE).astype(jnp.bfloat16)
            dv_acc[keys, :] += dot_f32(p.astype(jnp.bfloat16), do_ref[first:, :], PLAIN)
            dk_acc[keys, :] += dot_f32(ds, q_ref[first:, :], PLAIN)
            dqt_acc[:, first:] += dot_f32(kt_ref[:, keys], ds, PLAIN)

        now = scores(0)
        for b in range(0, rows, SUB):
            ahead = scores(b + SUB) if b + SUB < rows else None
            update(b, *now)
            now = ahead

    lax.fori_loop(0, i, lambda j, c: (step(j, False), c)[1], 0)
    step(i, True)

    @pl.when(i == 0)
    def _():
        for fetch in fetches:
            fetch.wait()

    tile = pl.ds(pl.multiple_of(i * rows, rows), rows)
    g_ref[tile, :HEAD_DIM] = unrope(dqt_acc[...].T, cos_buf[tile, :], sin_buf[tile, :])

    @pl.when(i == pl.num_programs(0) - 1)
    def _():
        def finish(j, c):
            part = pl.ds(pl.multiple_of(j * rows, rows), rows)
            g_ref[part, HEAD_DIM:2 * HEAD_DIM] = unrope(dk_acc[part, :], cos_buf[part, :], sin_buf[part, :])
            g_ref[part, 2 * HEAD_DIM:] = dv_acc[part, :].astype(jnp.bfloat16)
            return c

        lax.fori_loop(0, dk_acc.shape[0] // rows, finish, 0)


def attn_backward(q, do, ot, lse, k, v, kt, cos_full, sin_full, block, head):
    rows = q.shape[0]
    flops = 2 * rows * rows * HEAD_DIM // 2
    q_spec = pl.BlockSpec((block, HEAD_DIM), lambda i: (i, head))
    all_spec = pl.BlockSpec((rows, HEAD_DIM), lambda i: (0, head))
    table = pl.BlockSpec(memory_space=pl.ANY)
    return pl.pallas_call(
        bwd_kernel, grid=(rows // block,),
        in_specs=[q_spec, q_spec,
                  pl.BlockSpec((HEAD_DIM, block), lambda i: (head, i)),
                  pl.BlockSpec((1, 1, block), lambda i: (head, 0, i)),
                  all_spec, all_spec,
                  pl.BlockSpec((HEAD_DIM, rows), lambda i: (head, 0)),
                  table, table],
        out_specs=pl.BlockSpec((rows, 3 * HEAD_DIM), lambda i: (0, 0)),
        out_shape=jax.ShapeDtypeStruct((rows, 3 * HEAD_DIM), jnp.bfloat16),
        scratch_shapes=[pltpu.VMEM((rows, HEAD_DIM), jnp.float32),
                        pltpu.VMEM((rows, HEAD_DIM), jnp.float32),
                        pltpu.VMEM((HEAD_DIM, block), jnp.float32),
                        pltpu.VMEM((rows, HEAD_DIM), jnp.float32),
                        pltpu.VMEM((rows, HEAD_DIM), jnp.float32),
                        pltpu.SemaphoreType.DMA((2,))],
        compiler_params=pltpu.CompilerParams(vmem_limit_bytes=VMEM_LIMIT),
        cost_estimate=pl.CostEstimate(flops=2 * 5 * flops, bytes_accessed=20 * rows * HEAD_DIM, transcendentals=0),
        name="attn_bwd",
    )(q, do, ot, lse, k, v, kt, cos_full, sin_full)


def cot_kernel(g_ref, w_ref, ot_ref, do_ref, dw_ref, acc_ref):
    t = pl.program_id(0)

    @pl.when(t == 0)
    def _():
        acc_ref[...] = jnp.zeros_like(acc_ref)

    g = g_ref[...]
    do_ref[...] = dot_f32(g, w_ref[...], LAST).astype(jnp.bfloat16)
    acc_ref[...] += dot_f32(ot_ref[...].astype(jnp.bfloat16), g, PLAIN)

    @pl.when(t == pl.num_programs(0) - 1)
    def _():
        dw_ref[...] = acc_ref[...].astype(jnp.bfloat16)


def cotangents(g_all, wo_my, ot, block):
    rows, width = g_all.shape
    cols = wo_my.shape[0]
    slab = pl.BlockSpec((cols, width), lambda t: (0, 0))
    return pl.pallas_call(
        cot_kernel, grid=(rows // block,),
        in_specs=[pl.BlockSpec((block, width), lambda t: (t, 0)), slab, pl.BlockSpec((cols, block), lambda t: (0, t))],
        out_specs=[pl.BlockSpec((block, cols), lambda t: (t, 0)), slab],
        out_shape=[jax.ShapeDtypeStruct((rows, cols), jnp.bfloat16), jax.ShapeDtypeStruct((cols, width), jnp.bfloat16)],
        scratch_shapes=[pltpu.VMEM((cols, width), jnp.float32)],
        compiler_params=pltpu.CompilerParams(vmem_limit_bytes=VMEM_LIMIT),
        cost_estimate=pl.CostEstimate(flops=4 * rows * cols * width, bytes_accessed=2 * rows * (width + 3 * cols), transcendentals=0),
        name="cotangents",
    )(g_all, wo_my, ot)


def out_kernel(o_ref, w_ref, slab_ref, a_ref, dwo_ref, acc_ref):
    d = pl.program_id(0)
    dwo_ref[...] = slab_ref[...]

    @pl.when(d == 0)
    def _():
        acc_ref[...] = jnp.zeros_like(acc_ref)

    acc_ref[...] += dot_f32(o_ref[0], w_ref[...], PLAIN)

    @pl.when(d == pl.num_programs(0) - 1)
    def _():
        a_ref[...] = acc_ref[...].astype(jnp.bfloat16)


def out_project(o_chunks, w_o, dwo_slab):
    n, rows, cols = o_chunks.shape
    width = w_o.shape[1]
    return pl.pallas_call(
        out_kernel, grid=(n,),
        in_specs=[pl.BlockSpec((1, rows, cols), lambda d: (d, 0, 0)),
                  pl.BlockSpec((cols, width), lambda d: (d, 0)),
                  pl.BlockSpec((cols, width), lambda d: (d, 0))],
        out_specs=[pl.BlockSpec((rows, width), lambda d: (0, 0)),
                   pl.BlockSpec((cols, width), lambda d: (d, 0))],
        out_shape=[jax.ShapeDtypeStruct((rows, width), jnp.bfloat16),
                   jax.ShapeDtypeStruct(w_o.shape, jnp.bfloat16)],
        scratch_shapes=[pltpu.VMEM((rows, width), jnp.float32)],
        compiler_params=pltpu.CompilerParams(vmem_limit_bytes=VMEM_LIMIT),
        cost_estimate=pl.CostEstimate(flops=2 * n * rows * cols * width, bytes_accessed=2 * n * cols * (rows + width), transcendentals=0),
        name="out_project",
    )(o_chunks, w_o, dwo_slab)


def add_head(g_ref, wq_ref, wk_ref, wv_ref, acc_ref):
    w_qk = jnp.concatenate([wq_ref[...], wk_ref[...]], axis=1)
    acc_ref[...] += (dot_f32(g_ref[0, :, :2 * HEAD_DIM], w_qk, LAST)
                     + dot_f32(g_ref[0, :, 2 * HEAD_DIM:], wv_ref[...], LAST))


def tail_a_kernel(g_ref, wq_ref, wk_ref, wv_ref, dh_ref):
    @pl.when(pl.program_id(0) == 0)
    def _():
        dh_ref[...] = jnp.zeros_like(dh_ref)

    add_head(g_ref, wq_ref, wk_ref, wv_ref, dh_ref)


def tail_b_kernel(g_ref, wq_ref, wk_ref, wv_ref, first_ref, x_ref, lnw_ref, dx_ref, dlnw_ref, acc_ref, first_buf, x_buf, sems):
    d = pl.program_id(0)
    fetches = [pltpu.make_async_copy(first_ref, first_buf, sems.at[0]), pltpu.make_async_copy(x_ref, x_buf, sems.at[1])]

    @pl.when(d == 0)
    def _():
        for fetch in fetches:
            fetch.start()
        acc_ref[...] = jnp.zeros_like(acc_ref)

    add_head(g_ref, wq_ref, wk_ref, wv_ref, acc_ref)

    @pl.when(d == pl.num_programs(0) - 1)
    def _():
        for fetch in fetches:
            fetch.wait()
        dlnw_ref[...] = jnp.zeros_like(dlnw_ref)
        lnw = lnw_ref[...]
        step = 64

        def rows_step(t, c):
            rows = pl.ds(pl.multiple_of(t * step, step), step)
            x = x_buf[rows, :].astype(jnp.float32)
            dh = acc_ref[rows, :] + first_buf[rows, :]
            centered = x - jnp.mean(x, axis=-1, keepdims=True)
            rstd = lax.rsqrt(jnp.mean(centered * centered, axis=-1, keepdims=True) + LN_EPS)
            xhat = centered * rstd
            dlnw_ref[...] += jnp.sum(dh * xhat, axis=0, keepdims=True)
            dxhat = dh * lnw
            dx = rstd * (dxhat - jnp.mean(dxhat, axis=-1, keepdims=True) - xhat * jnp.mean(dxhat * xhat, axis=-1, keepdims=True))
            dx_ref[rows, :] = dx.astype(jnp.bfloat16)
            return c

        lax.fori_loop(0, x_buf.shape[0] // step, rows_step, 0)


def tail(g_chunks, w_q, w_k, w_v, head, heads, rest=()):
    n, rows, cols = g_chunks.shape
    width = w_q.shape[0]
    w_spec = pl.BlockSpec((width, HEAD_DIM), lambda d: (0, heads * d + head))
    whole = pl.BlockSpec((rows, width), lambda d: (0, 0))
    row = pl.BlockSpec((1, width), lambda d: (0, 0))
    dh = jax.ShapeDtypeStruct((rows, width), jnp.float32)
    last = bool(rest)
    return pl.pallas_call(
        tail_b_kernel if last else tail_a_kernel, grid=(n,),
        in_specs=[pl.BlockSpec((1, rows, cols), lambda d: (d, 0, 0)), w_spec, w_spec, w_spec] + ([pl.BlockSpec(memory_space=pl.ANY)] * 2 + [row] if last else []),
        out_specs=[whole, row] if last else whole,
        out_shape=[jax.ShapeDtypeStruct((rows, width), jnp.bfloat16), jax.ShapeDtypeStruct((1, width), jnp.float32)] if last else dh,
        scratch_shapes=[pltpu.VMEM((rows, width), jnp.float32), pltpu.VMEM((rows, width), jnp.float32),
                        pltpu.VMEM((rows, width), jnp.bfloat16), pltpu.SemaphoreType.DMA((2,))] if last else [],
        compiler_params=pltpu.CompilerParams(vmem_limit_bytes=VMEM_LIMIT),
        cost_estimate=pl.CostEstimate(flops=2 * n * rows * cols * width, bytes_accessed=2 * n * cols * (rows + width), transcendentals=0),
        name="tail_b" if last else "tail_a",
    )(g_chunks, w_q, w_k, w_v, *rest)


def assemble_kernel(slab_ref, *refs):
    for part, out in enumerate(refs[-3:]):
        out[...] = slab_ref[0, :, part * HEAD_DIM:(part + 1) * HEAD_DIM]


def assemble(slab, head, heads, into=()):
    n, rows, cols = slab.shape
    out_spec = pl.BlockSpec((rows, HEAD_DIM), lambda d: (0, heads * d + head))
    out = jax.ShapeDtypeStruct((rows, n * heads * HEAD_DIM), jnp.bfloat16)
    return pl.pallas_call(
        assemble_kernel, grid=(n,),
        in_specs=[pl.BlockSpec((1, rows, cols), lambda d: (d, 0, 0))] + [pl.BlockSpec(memory_space=pl.ANY)] * len(into),
        out_specs=[out_spec] * 3, out_shape=[out] * 3,
        input_output_aliases={1 + i: i for i in range(len(into))},
        compiler_params=pltpu.CompilerParams(vmem_limit_bytes=VMEM_LIMIT),
        cost_estimate=pl.CostEstimate(flops=rows * n * cols * 64, bytes_accessed=4 * n * rows * cols, transcendentals=0),
        name="assemble",
    )(slab, *into)


def solution(mesh):
    sp_size = mesh.shape['sp']
    row_spec = P(('dp', 'sp'), None)
    pos_spec = P(('dp', 'sp'))
    full_spec = P(None, None)
    grad_spec = P('dp', None)

    def layer(hidden, positions, d_attn, ln_weight, w_q, w_k, w_v, w_o):
        me = lax.axis_index('sp')
        block = hidden.shape[0]
        cols = w_q.shape[1] // sp_size
        lnw32 = ln_weight.astype(jnp.float32)
        normed = layer_norm(hidden, lnw32[None])
        pos_all = lax.all_gather(positions, 'sp', tiled=True)
        h_all = lax.all_gather(normed, 'sp', tiled=True)
        g_all = lax.all_gather(d_attn, 'sp', tiled=True)
        cos_full, sin_full = rope_tables(pos_all)
        mine = lambda w, axis: lax.dynamic_slice_in_dim(w, me * cols, cols, axis)
        wq_my, wk_my, wv_my, wo_my = mine(w_q, 1), mine(w_k, 1), mine(w_v, 1), mine(w_o, 0)
        q, k, v, kt, vt = project(h_all, wq_my, wk_my, wv_my, cos_full, sin_full)

        def exchange(x):
            return lax.all_to_all(x.reshape(sp_size, block, x.shape[1]), 'sp', 0, 0)

        o, ot, lse = attn_forward(q, k, vt, block)
        o_chunks = exchange(o)
        d_o, dwo_my = cotangents(g_all, wo_my, ot, block)

        def back(q, head):
            return attn_backward(q, d_o, ot, lse, k, v, kt, cos_full, sin_full, block, head)

        def wgrad(x):
            return jnp.einsum('td,te->de', h_all, x, preferred_element_type=jnp.float32).astype(jnp.bfloat16)

        q_0, dwo_my = lax.optimization_barrier((q, dwo_my))
        dwo_slab = lax.all_gather(dwo_my, 'sp', tiled=True)
        g_a = back(q_0, 0)
        sent_a, o_chunks = lax.optimization_barrier((g_a, o_chunks))
        ga_tok = exchange(sent_a)
        q_1, part_a = lax.optimization_barrier((q, wgrad(g_a)))
        slab_a = lax.all_gather(part_a, 'sp')
        g_b = back(q_1, 1)
        sent_b, ga_tok = lax.optimization_barrier((g_b, ga_tok))
        gb_tok = exchange(sent_b)
        part_b = wgrad(g_b)
        slab_b = lax.all_gather(part_b, 'sp')
        ga_tok, o_chunks, dwo_slab, part_b = lax.optimization_barrier((ga_tok, o_chunks, dwo_slab, part_b))
        dh_a = tail(ga_tok, w_q, w_k, w_v, 0, 2)
        attn_out, dw_o = out_project(o_chunks, w_o, dwo_slab)
        dh_a, attn_out, dw_o, slab_a = lax.optimization_barrier((dh_a, attn_out, dw_o, slab_a))
        half = assemble(slab_a, 0, 2)
        d_hid, d_lnw = tail(gb_tok, w_q, w_k, w_v, 1, 2, (dh_a, hidden, lnw32[None]))
        parts = lax.all_to_all(jnp.broadcast_to(d_lnw[None], (sp_size,) + d_lnw.shape), 'sp', 0, 0)
        d_lnw = jnp.sum(parts, axis=(0, 1)).astype(jnp.bfloat16)
        half, d_hid, attn_out, slab_b = lax.optimization_barrier((half, d_hid, attn_out, slab_b))
        dw_q, dw_k, dw_v = assemble(slab_b, 1, 2, half)
        return attn_out, d_hid, d_lnw, dw_q, dw_k, dw_v, dw_o

    return jax.shard_map(layer, mesh=mesh,
                         in_specs=(row_spec, pos_spec, row_spec, P(None), full_spec, full_spec, full_spec, full_spec),
                         out_specs=(row_spec, row_spec, P('dp'), grad_spec, grad_spec, grad_spec, grad_spec),
                         check_vma=False)
```
